32 devices in a mesh: pts: 8 (over z, y), hrs: 4 (over x, core).
Axes of the slice: x: 2, y: 2, z: 4, core: 2. Of those that a mesh axis runs over, the one named last changes fastest.
Arguments:
- fields: float32 [512, 65536], P(('pts', 'hrs')), may hold values from -2000 to 2000, as said below
- probes: float32 [256, 512], replicated, may hold values from -0.25 to 0.25
Outputs:
- basis_rows: float32 [256, 65536], P(None, ('pts', 'hrs'))
- coeffs: float32 [256, 512], replicated
The draws below stay inside these ranges and needn't reach their ends.
Inputs may be any that keep to these rules, and one draw needn't show every extreme that they name: `fields`: every hour and every grid point carries its own scale, and the values are real-valued and never all zero.
All inputs are finite; a program needn't handle non-finite values.
Results may differ from the reference program's by a relative error of at most 0.00017.
Values sent between devices are 32-bit elements; how exact they have to be, the bound alone decides.
A program may use at most 64 MiB of HBM per device.

```python
import jax
import jax.numpy as jnp
from jax import lax

K = 256
HOURS = 512
POINTS = 65536


def draw_fields(key, part):
    keys_all = jax.random.split(jax.random.fold_in(key, 11), 3)
    point_scale = 10.0 ** jax.random.uniform(keys_all[1], (1, POINTS), dtype=jnp.float32)
    lat_ramp = 1.0 + 2.0 * jnp.arange(POINTS, dtype=jnp.float32)[None, :] / (POINTS - 1)
    hour_scale = 10.0 ** jax.random.uniform(keys_all[0], (HOURS, 1), dtype=jnp.float32)
    noise_part = jnp.clip(jax.random.normal(keys_all[2], (HOURS, POINTS), dtype=jnp.float32), -4.0, 4.0)
    return hour_scale * point_scale * lat_ramp * noise_part


def gaussian(own_key, extent, width, most, held_as=jnp.bfloat16):
    values = width * jax.random.normal(own_key, extent, jnp.float32)
    return jnp.clip(values, min=-most, max=most).astype(held_as)


def setup_inputs(seed: int = 0) -> dict:
    key_of = jax.random.split(jax.random.key(seed), 3)
    fields = draw_fields(jax.random.fold_in(key_of[2], 71), 0)
    probes = gaussian(key_of[1], (K, HOURS), HOURS ** -0.5, 0.25, jnp.float32)
    return {"fields": fields, "probes": probes}


highest = lax.Precision.HIGHEST

def reference(fields, probes):
    n_points = fields.shape[1]
    sketched = jnp.dot(probes.astype(jnp.float32), fields.astype(jnp.float32), precision=highest, preferred_element_type=jnp.float32)
    gram = lax.dot_general(sketched.astype(jnp.float32), sketched.astype(jnp.float32), (((1,), (1,)), ((), ())), precision=highest, preferred_element_type=jnp.float32) / n_points
    lower = jnp.linalg.cholesky(gram)
    basis_rows = lax.linalg.triangular_solve(lower, sketched, left_side=True, lower=True)
    coeffs = lax.dot_general(basis_rows.astype(jnp.float32), fields.astype(jnp.float32), (((1,), (1,)), ((), ())), precision=highest, preferred_element_type=jnp.float32) / n_points
    return (basis_rows, coeffs)
```

```python
import functools

import jax
import jax.numpy as jnp
from jax import lax
from jax.experimental import pallas as pl
from jax.experimental.pallas import tpu as pltpu
from jax.sharding import PartitionSpec as P

HI = lax.Precision.HIGHEST
MESH = pl.DeviceIdType.MESH


def mm(a, b, dims):
    return lax.dot_general(a, b, (dims, ((), ())), precision=HI, preferred_element_type=jnp.float32)


def invert_block(block):
    b = block.shape[0]
    n = b // 8
    shape = (8, b)
    srow = lax.broadcasted_iota(jnp.int32, shape, 0)
    lane = lax.broadcasted_iota(jnp.int32, shape, 1)
    strips = [block[8 * s:8 * s + 8] for s in range(n)]
    diag = sum(jnp.where(lane == srow + 8 * s, strips[s], 0.0) for s in range(n))
    diag = jnp.broadcast_to(jnp.sum(diag, axis=0, keepdims=True), shape)
    col = 1.0 / diag
    root = lax.rsqrt(diag)
    strips = [strip * col for strip in strips]
    outs = [jnp.zeros(shape, jnp.float32)] * n

    def row_of(x, r):
        return jnp.broadcast_to(x[r:r + 1], shape)

    def spread(x, c, apart=True):
        x = jnp.broadcast_to(x[:, c:c + 1], shape)
        return jnp.maximum(x, -3e38) if apart else x

    for s0 in range(n):
        j = 8 * s0
        panel = {s: [spread(strips[s], j + c, s == s0) for c in range(8)] for s in range(s0, n)}
        roots = [spread(root, j + c) for c in range(8)]
        inside = (lane >= j) & (lane < j + 8)
        for s in range(s0, n):
            unit = jnp.where(lane == srow + j, 1.0, 0.0) if s == s0 else 0.0
            strips[s] = jnp.where(inside, unit, strips[s])
        head = panel[s0]
        for p in range(0, 8, 2):
            a, b12 = row_of(head[p], p), row_of(head[p + 1], p)
            b21, c = row_of(head[p], p + 1), row_of(head[p + 1], p + 1)
            det = a * c - b12 * b21
            inv = 1.0 / det
            inva = 1.0 / a
            row1, row2 = row_of(strips[s0], p), row_of(strips[s0], p + 1)
            w1 = row1 * (lax.rsqrt(a) * roots[p])
            w2 = (row2 - (b21 * inva) * row1) * (lax.rsqrt(det * inva) * roots[p + 1])
            outs[s0] = jnp.where(srow == p, w1, jnp.where(srow == p + 1, w2, outs[s0]))
            v1, v2 = (c * row1 - b12 * row2) * inv, (a * row2 - b21 * row1) * inv
            y = {}
            for q in range(p + 2, 8):
                e1, e2 = row_of(head[q], p), row_of(head[q], p + 1)
                y[q] = (c * e1 - b12 * e2, a * e2 - b21 * e1)
            z = {q: (y[q][0] * inv, y[q][1] * inv) for q in y}
            for s in range(s0 if p < 6 else s0 + 1, n):
                f = panel[s]
                for q in range(p + 2, 8):
                    if s < s0 + 2:
                        f[q] = f[q] - (f[p] * y[q][0] + f[p + 1] * y[q][1]) * inv
                    else:
                        f[q] = f[q] - f[p] * z[q][0] - f[p + 1] * z[q][1]
                strips[s] = strips[s] - f[p] * v1 - f[p + 1] * v2
    return jnp.concatenate([jnp.where(lane <= srow + 8 * s, outs[s], 0.0) for s in range(n)], axis=0)


def factor(a, w, b):
    k = a.shape[0]
    for lo in range(0, k, b):
        hi = lo + b
        d = invert_block(a[lo:hi, lo:hi])
        if hi < k:
            lt = mm(d, a[lo:hi, hi:], ((1,), (0,)))
            a[hi:, hi:] = a[hi:, hi:] - mm(lt, lt, ((0,), (0,)))
            w[lo:hi, hi:] = jnp.zeros((b, k - hi), jnp.float32)
        w[lo:hi, lo:hi] = d
        if lo:
            w[lo:hi, :lo] = mm(d, w[lo:hi, :lo], ((1,), (0,)))
        if hi < k:
            t = mm(lt, w[lo:hi, :hi], ((0,), (0,)))
            if lo:
                w[hi:, :lo] = w[hi:, :lo] - t[:, :lo]
            w[hi:, lo:hi] = -t[:, lo:]


def finish_kernel(cross, probes, sk_hbm, basis, coeffs, gram, w, sk, y, sk_sem, out_sem):
    k = gram.shape[0]
    half = k // 2
    n = sk.shape[1]
    load = pltpu.make_async_copy(sk_hbm, sk, sk_sem)
    load.start()
    gram[...] = mm(cross[...], probes[...], ((1,), (1,)))
    factor(gram, w, half)
    load.wait()
    stores = []
    for i, (lo, hi) in enumerate(((0, half), (half, k))):
        for t in range(0, n, 512):
            y[lo:hi, t:t + 512] = mm(w[lo:hi, :hi], sk[:hi, t:t + 512], ((1,), (0,)))
        stores.append(pltpu.make_async_copy(y.at[lo:hi], basis.at[lo:hi], out_sem.at[i]))
        stores[-1].start()
        coeffs[lo:hi, :] = mm(w[lo:hi, :hi], cross[:hi, :], ((1,), (0,)))
    for store in stores:
        store.wait()


def finish(cross, probes, sk):
    k = cross.shape[0]
    v = pl.BlockSpec(memory_space=pltpu.VMEM)
    hbm = pl.BlockSpec(memory_space=pl.ANY)
    f32 = jnp.float32
    return pl.pallas_call(
        finish_kernel,
        out_shape=(jax.ShapeDtypeStruct(sk.shape, f32), jax.ShapeDtypeStruct(cross.shape, f32)),
        in_specs=[v, v, hbm],
        out_specs=(hbm, v),
        scratch_shapes=[
            pltpu.VMEM((k, k), f32), pltpu.VMEM((k, k), f32), pltpu.VMEM(sk.shape, f32), pltpu.VMEM(sk.shape, f32),
            pltpu.SemaphoreType.DMA(()), pltpu.SemaphoreType.DMA((2,)),
        ],
        name="factor",
    )(cross, probes, sk)


class Place:
    def __init__(self, n_pts, n_hrs):
        self.pts, self.hrs = lax.axis_index("pts"), lax.axis_index("hrs")
        self.n_pts, self.n_hrs = n_pts, n_hrs
        self.cores, self.low, self.chips, self.layers = split(n_pts, n_hrs)
        self.core = lax.rem(self.hrs, self.cores)
        self.layer = self.pts // self.low
        self.chip = (self.hrs // self.cores) * self.low + lax.rem(self.pts, self.low)

    def at(self, core, chip, layer):
        return (layer * self.low + lax.rem(chip, self.low), (chip // self.low) * self.cores + core)


def split(n_pts, n_hrs):
    cores = 2 if n_hrs % 2 == 0 else 1
    low = 1
    while n_pts % (low * 2) == 0 and low * 2 * low * 2 <= n_pts:
        low *= 2
    return cores, low, (n_hrs // cores) * low, n_pts // low


def reduce_shapes(n_pts, n_hrs, rows, width, parts):
    cores, low, chips, layers = split(n_pts, n_hrs)
    lanes = width // cores
    h = rows // parts
    q = h // chips
    f32 = jnp.float32
    dma = pltpu.SemaphoreType.DMA
    return [
        pltpu.VMEM((parts, h, lanes), f32),
        pltpu.VMEM((parts, h, lanes), f32),
        pltpu.VMEM((parts, max(chips - 1, 1), q, lanes), f32),
        pltpu.VMEM((parts, layers, q, lanes), f32),
        dma((parts, 2)), dma((parts, 2)),
        dma((parts, 2, max(chips - 1, 1))), dma((parts, 2, max(chips - 1, 1))),
        dma((parts, max(layers - 1, 1))), dma((parts, max(layers - 1, 1))),
    ]


class AllReduce:
    def __init__(self, place, x, out, parts, scale, scratch):
        self.place, self.x, self.out, self.parts, self.scale = place, x, out, parts, scale
        self.got1, self.sum1, self.got2, self.sums, self.s1, self.r1, self.s2, self.r2, self.s3, self.r3 = scratch
        self.h, self.lanes = self.got1.shape[1], self.got1.shape[2]
        self.q = self.sums.shape[2]
        self.started = []
        self.copies = {}

    def send(self, key, src, dst, ss, rs, device):
        copy = pltpu.make_async_remote_copy(
            src_ref=src, dst_ref=dst, send_sem=ss, recv_sem=rs, device_id=device, device_id_type=MESH)
        copy.start()
        self.started.append(copy)
        self.copies.setdefault(key, []).append(copy)

    def arrived(self, key):
        for copy in self.copies.get(key, ()):
            copy.wait_recv()

    def half(self, core, p):
        return pl.ds(p * self.h, self.h), pl.ds(pl.multiple_of(core * self.lanes, 128), self.lanes)

    def piece(self, chip):
        return pl.ds(pl.multiple_of(chip * self.q, 8), self.q)

    def cores(self, p):
        at = self.place
        if at.cores > 1:
            other = 1 - at.core
            self.send((1, p), self.x.at[self.half(other, p)], self.got1.at[p], self.s1.at[p, 0], self.r1.at[p, 0],
                      at.at(other, at.chip, at.layer))

    def chips(self, p):
        at = self.place
        self.arrived((1, p))
        mine = self.x[self.half(at.core, p)]
        self.sum1[p] = mine + self.got1[p] if at.cores > 1 else mine
        for o in range(1, at.chips):
            chip = lax.rem(at.chip + o, at.chips)
            self.send((2, p), self.sum1.at[p, self.piece(chip)], self.got2.at[p, o - 1], self.s2.at[p, 0, o - 1], self.r2.at[p, 0, o - 1],
                      at.at(at.core, chip, at.layer))

    def layers(self, p):
        at = self.place
        self.arrived((2, p))
        total = self.sum1[p, self.piece(at.chip)]
        for o in range(1, at.chips):
            total = total + self.got2[p, o - 1]
        self.sums[p, at.layer] = total
        for o in range(1, at.layers):
            layer = lax.rem(at.layer + o, at.layers)
            self.send((3, p), self.sums.at[p, at.layer], self.sums.at[p, at.layer], self.s3.at[p, o - 1], self.r3.at[p, o - 1],
                      at.at(at.core, at.chip, layer))

    def spread(self, p):
        at = self.place
        self.arrived((3, p))
        total = self.sums[p, 0]
        for layer in range(1, at.layers):
            total = total + self.sums[p, layer]
        rows, lanes = self.half(at.core, p)
        block = (pl.ds(pl.multiple_of(p * self.h + at.chip * self.q, 8), self.q), lanes)
        self.out[block] = total * self.scale
        for o in range(1, at.chips):
            chip = lax.rem(at.chip + o, at.chips)
            self.send((4, p), self.out.at[block], self.out.at[block], self.s2.at[p, 1, o - 1], self.r2.at[p, 1, o - 1],
                      at.at(at.core, chip, at.layer))

    def share(self, p):
        at = self.place
        self.arrived((4, p))
        if at.cores > 1:
            half = self.half(at.core, p)
            self.send((5, p), self.out.at[half], self.out.at[half], self.s1.at[p, 1], self.r1.at[p, 1],
                      at.at(1 - at.core, at.chip, at.layer))

    def run(self, step):
        for p in range(self.parts):
            step(p)

    def finish(self):
        for p in range(self.parts):
            self.arrived((5, p))

    def drain(self):
        for copy in self.started:
            copy.wait_send()


def gather_kernel(n_pts, n_hrs, widths, parts, n_points, fields_ref, probes_ref, sk_hbm, cross_ref, *scratch):
    n = n_pts * n_hrs
    m = len(widths)
    panels, scratch = scratch[:m], scratch[m:]
    flat, part, sk, own_sem, send_sem, recv_sem, sk_sem, *scratch = scratch
    place = Place(n_pts, n_hrs)
    me = place.pts * n_hrs + place.hrs
    rows = fields_ref.shape[0]
    local = sum(widths)
    k, hours = part.shape

    def split_id(o):
        t = lax.rem(me + o, n)
        return t, t // n_hrs, lax.rem(t, n_hrs)

    barrier = pltpu.get_barrier_semaphore()

    @pl.loop(1, n)
    def _(o):
        _, tp, th = split_id(o)
        pl.semaphore_signal(barrier, inc=1, device_id=(tp, th), device_id_type=MESH)

    pl.semaphore_wait(barrier, n - 1)

    starts = [sum(widths[:c]) for c in range(m)]

    def source(t, c):
        return fields_ref.at[:, pl.ds(pl.multiple_of(t * local + starts[c], 128), widths[c])]

    owns = []
    for c in range(m):
        @pl.loop(1, n)
        def _(o):
            t, tp, th = split_id(o)
            pltpu.make_async_remote_copy(
                src_ref=source(t, c), dst_ref=panels[c].at[me], send_sem=send_sem.at[c], recv_sem=recv_sem.at[c],
                device_id=(tp, th), device_id_type=MESH,
            ).start()

        own = pltpu.make_async_copy(source(me, c), panels[c].at[me], own_sem.at[c])
        own.start()
        owns.append(own)

    reduce = AllReduce(place, part, cross_ref, parts, 1.0 / n_points, scratch)
    stores = []
    for c in range(m):
        owns[c].wait()
        most = panels[c].at[pl.ds(0, n - 1)]
        pltpu.make_async_copy(most, most, recv_sem.at[c]).wait()
        width = widths[c]
        cols = pl.ds(starts[c], width)
        if rows % 8 == 0:
            block = panels[c][...].reshape(n * rows, width)
        else:
            for d in range(n):
                flat[d * rows:(d + 1) * rows, :width] = panels[c][d]
            block = flat[:, :width]
        sk[:, cols] = mm(probes_ref[...], block, ((1,), (0,)))
        term = mm(sk[:, cols], block, ((1,), (1,)))
        part[...] = term if c == 0 else part[...] + term
        stores.append(pltpu.make_async_copy(sk.at[:, cols], sk_hbm.at[:, cols], sk_sem.at[c]))
        if c < m - 1:
            stores[-1].start()
    reduce.run(reduce.cores)
    stores[-1].start()
    reduce.run(reduce.chips)
    reduce.run(reduce.layers)
    reduce.run(reduce.spread)
    reduce.run(reduce.share)
    reduce.finish()
    reduce.drain()
    for store in stores:
        store.wait()
    for c in range(m):
        most = panels[c].at[pl.ds(0, n - 1)]
        pltpu.make_async_copy(most, most, send_sem.at[c]).wait()


def gather(fields, probes, n_pts, n_hrs):
    k, hours = probes.shape
    rows, n_points = fields.shape
    n = n_pts * n_hrs
    local = n_points // n
    widths = pieces(local)
    m = len(widths)
    cores, low, chips, layers = split(n_pts, n_hrs)
    parts = 2 if k % (2 * chips * 8) == 0 else 1
    v = pl.BlockSpec(memory_space=pltpu.VMEM)
    hbm = pl.BlockSpec(memory_space=pl.ANY)
    dma = pltpu.SemaphoreType.DMA
    f32 = jnp.float32
    return pl.pallas_call(
        functools.partial(gather_kernel, n_pts, n_hrs, widths, parts, n_points),
        out_shape=(jax.ShapeDtypeStruct((k, local), f32), jax.ShapeDtypeStruct((k, hours), f32)),
        in_specs=[hbm, v],
        out_specs=(hbm, v),
        scratch_shapes=[
            *(pltpu.VMEM((n, rows, width), f32) for width in widths),
            pltpu.VMEM((hours, max(widths)) if rows % 8 else (8, 128), f32),
            pltpu.VMEM((k, hours), f32),
            pltpu.VMEM((k, local), f32),
            dma((m,)), dma((m,)), dma((m,)), dma((m,)),
            *reduce_shapes(n_pts, n_hrs, k, hours, parts),
        ],
        compiler_params=pltpu.CompilerParams(collective_id=1, has_side_effects=True),
        name="gather",
    )(fields, probes)


def pieces(local):
    if local % 128 or local < 1024:
        return (local,)
    last = 128
    big = 512
    rest = local - last
    widths = []
    while rest > big:
        widths.append(big)
        rest -= big
    return (*widths, rest, last)


def on_device(fields, probes):
    n_pts = lax.axis_size("pts")
    n_hrs = lax.axis_size("hrs")
    sketched, cross = gather(fields, probes, n_pts, n_hrs)
    return finish(cross, probes, sketched)


def solution(mesh):
    return jax.shard_map(
        on_device,
        mesh=mesh,
        in_specs=(P(("pts", "hrs"), None), P()),
        out_specs=(P(None, ("pts", "hrs")), P()),
        check_vma=False,
    )
```

```python
import functools

import jax
import jax.numpy as jnp
from jax import lax
from jax.experimental import pallas as pl
from jax.experimental.pallas import tpu as pltpu
from jax.sharding import PartitionSpec as P

HI = lax.Precision.HIGHEST
MESH = pl.DeviceIdType.MESH
POINTS = ((0, 0), (0, 6), (1, 2), (1, 13))


def mm(a, b, dims):
    return lax.dot_general(a, b, (dims, ((), ())), precision=HI, preferred_element_type=jnp.float32)


def invert_block(block, between=None):
    b = block.shape[0]
    n = b // 8
    shape = (8, b)
    srow = lax.broadcasted_iota(jnp.int32, shape, 0)
    lane = lax.broadcasted_iota(jnp.int32, shape, 1)
    strips = [block[8 * s:8 * s + 8] for s in range(n)]
    diag = sum(jnp.where(lane == srow + 8 * s, strips[s], 0.0) for s in range(n))
    diag = jnp.broadcast_to(jnp.sum(diag, axis=0, keepdims=True), shape)
    col = 1.0 / diag
    root = lax.rsqrt(diag)
    strips = [strip * col for strip in strips]
    outs = [jnp.zeros(shape, jnp.float32)] * n

    def row_of(x, r):
        return jnp.broadcast_to(x[r:r + 1], shape)

    def spread(x, c, apart=True):
        x = jnp.broadcast_to(x[:, c:c + 1], shape)
        return jnp.maximum(x, -3e38) if apart else x

    for s0 in range(n):
        j = 8 * s0
        if between is not None:
            between(s0)
        panel = {s: [spread(strips[s], j + c, s == s0) for c in range(8)] for s in range(s0, n)}
        roots = [spread(root, j + c) for c in range(8)]
        inside = (lane >= j) & (lane < j + 8)
        for s in range(s0, n):
            unit = jnp.where(lane == srow + j, 1.0, 0.0) if s == s0 else 0.0
            strips[s] = jnp.where(inside, unit, strips[s])
        head = panel[s0]
        for p in range(0, 8, 2):
            a, b12 = row_of(head[p], p), row_of(head[p + 1], p)
            b21, c = row_of(head[p], p + 1), row_of(head[p + 1], p + 1)
            det = a * c - b12 * b21
            inv = 1.0 / det
            inva = 1.0 / a
            row1, row2 = row_of(strips[s0], p), row_of(strips[s0], p + 1)
            w1 = row1 * (lax.rsqrt(a) * roots[p])
            w2 = (row2 - (b21 * inva) * row1) * (lax.rsqrt(det * inva) * roots[p + 1])
            outs[s0] = jnp.where(srow == p, w1, jnp.where(srow == p + 1, w2, outs[s0]))
            v1, v2 = (c * row1 - b12 * row2) * inv, (a * row2 - b21 * row1) * inv
            y = {}
            for q in range(p + 2, 8):
                e1, e2 = row_of(head[q], p), row_of(head[q], p + 1)
                y[q] = (c * e1 - b12 * e2, a * e2 - b21 * e1)
            z = {q: (y[q][0] * inv, y[q][1] * inv) for q in y}
            for s in range(s0 if p < 6 else s0 + 1, n):
                f = panel[s]
                for q in range(p + 2, 8):
                    if s < s0 + 2:
                        f[q] = f[q] - (f[p] * y[q][0] + f[p + 1] * y[q][1]) * inv
                    else:
                        f[q] = f[q] - f[p] * z[q][0] - f[p + 1] * z[q][1]
                strips[s] = strips[s] - f[p] * v1 - f[p + 1] * v2
    return jnp.concatenate([jnp.where(lane <= srow + 8 * s, outs[s], 0.0) for s in range(n)], axis=0)


def packed(k, chips, parts):
    step = 8 * chips * parts
    return -(-(k // 2 + k // 4) // step) * step


def pack(g, gram, first):
    k = gram.shape[1]
    h, q = k // 2, k // 4
    for rows, cols, block in (
        (slice(0, h), slice(0, h), g[:h, :h]),
        (slice(0, h), slice(h, k), g[h:, h:]),
        (slice(h, h + q), slice(0, h), g[h:h + q, :h]),
        (slice(h, h + q), slice(h, k), g[h + q:, :h]),
    ):
        gram[rows, cols] = block if first else gram[rows, cols] + block


def factor(gram, w, between):
    k = w.shape[0]
    h, q = k // 2, k // 4
    top = invert_block(gram[:h, :h], functools.partial(between, 0))
    w[:h, :h] = top
    w[:h, h:] = jnp.zeros((h, k - h), jnp.float32)
    below = jnp.concatenate([gram[h:h + q, :h], gram[h:h + q, h:]], axis=0)
    side = mm(below, top, ((1,), (1,)))
    rest = gram[:h, h:] - mm(side, side, ((1,), (1,)))
    w[h:, :h] = mm(side, top, ((1,), (0,)))
    last = invert_block(rest, functools.partial(between, 1))
    w[h:, h:] = last
    w[h:, :h] = -mm(last, w[h:, :h], ((1,), (0,)))


def apply_kernel(w, cross, sk_hbm, basis, coeffs, sk, y, sk_sem, out_sem):
    n = sk.shape[1]
    step = 512
    loads, stores = [], []
    for t in range(0, n, step):
        loads.append(pltpu.make_async_copy(sk_hbm.at[:, t:t + step], sk.at[:, t:t + step], sk_sem.at[len(loads)]))
        loads[-1].start()
    for i, t in enumerate(range(0, n, step)):
        loads[i].wait()
        y[:, t:t + step] = mm(w[...], sk[:, t:t + step], ((1,), (0,)))
        stores.append(pltpu.make_async_copy(y.at[:, t:t + step], basis.at[:, t:t + step], out_sem.at[i]))
        stores[-1].start()
        if i == 0:
            coeffs[...] = mm(w[...], cross[...], ((1,), (0,)))
    for store in stores:
        store.wait()


def finish(w, cross, sk):
    v = pl.BlockSpec(memory_space=pltpu.VMEM)
    hbm = pl.BlockSpec(memory_space=pl.ANY)
    f32 = jnp.float32
    count = -(-sk.shape[1] // 512)
    return pl.pallas_call(
        apply_kernel,
        out_shape=(jax.ShapeDtypeStruct(sk.shape, f32), jax.ShapeDtypeStruct(cross.shape, f32)),
        in_specs=[v, v, hbm],
        out_specs=(hbm, v),
        scratch_shapes=[
            pltpu.VMEM(sk.shape, f32), pltpu.VMEM(sk.shape, f32),
            pltpu.SemaphoreType.DMA((count,)), pltpu.SemaphoreType.DMA((count,)),
        ],
        name="apply",
    )(w, cross, sk)


class Place:
    def __init__(self, n_pts, n_hrs):
        self.pts, self.hrs = lax.axis_index("pts"), lax.axis_index("hrs")
        self.n_pts, self.n_hrs = n_pts, n_hrs
        self.cores, self.low, self.chips, self.layers = split(n_pts, n_hrs)
        self.core = lax.rem(self.hrs, self.cores)
        self.layer = self.pts // self.low
        self.chip = (self.hrs // self.cores) * self.low + lax.rem(self.pts, self.low)

    def at(self, core, chip, layer):
        return (layer * self.low + lax.rem(chip, self.low), (chip // self.low) * self.cores + core)


def split(n_pts, n_hrs):
    cores = 2 if n_hrs % 2 == 0 else 1
    low = 1
    while n_pts % (low * 2) == 0 and low * 2 * low * 2 <= n_pts:
        low *= 2
    return cores, low, (n_hrs // cores) * low, n_pts // low


def reduce_shapes(n_pts, n_hrs, rows, width, parts):
    cores, low, chips, layers = split(n_pts, n_hrs)
    lanes = width // cores
    h = rows // parts
    q = h // chips
    f32 = jnp.float32
    dma = pltpu.SemaphoreType.DMA
    return [
        pltpu.VMEM((parts, h, lanes), f32),
        pltpu.VMEM((parts, h, lanes), f32),
        pltpu.VMEM((parts, max(chips - 1, 1), q, lanes), f32),
        pltpu.VMEM((parts, layers, q, lanes), f32),
        dma((parts, 2)), dma((parts, 2)),
        dma((parts, 2, max(chips - 1, 1))), dma((parts, 2, max(chips - 1, 1))),
        dma((parts, max(layers - 1, 1))), dma((parts, max(layers - 1, 1))),
    ]


class AllReduce:
    def __init__(self, place, x, out, parts, scale, scratch):
        self.place, self.x, self.out, self.parts, self.scale = place, x, out, parts, scale
        self.got1, self.sum1, self.got2, self.sums, self.s1, self.r1, self.s2, self.r2, self.s3, self.r3 = scratch
        self.h, self.lanes = self.got1.shape[1], self.got1.shape[2]
        self.q = self.sums.shape[2]
        self.started = []
        self.copies = {}

    def send(self, key, src, dst, ss, rs, device):
        copy = pltpu.make_async_remote_copy(
            src_ref=src, dst_ref=dst, send_sem=ss, recv_sem=rs, device_id=device, device_id_type=MESH)
        copy.start()
        self.started.append(copy)
        self.copies.setdefault(key, []).append(copy)

    def arrived(self, key):
        for copy in self.copies.get(key, ()):
            copy.wait_recv()

    def half(self, core, p):
        return pl.ds(p * self.h, self.h), pl.ds(pl.multiple_of(core * self.lanes, 128), self.lanes)

    def piece(self, chip):
        return pl.ds(pl.multiple_of(chip * self.q, 8), self.q)

    def cores(self, p):
        at = self.place
        if at.cores > 1:
            other = 1 - at.core
            self.send((1, p), self.x.at[self.half(other, p)], self.got1.at[p], self.s1.at[p, 0], self.r1.at[p, 0],
                      at.at(other, at.chip, at.layer))

    def chips(self, p):
        at = self.place
        self.arrived((1, p))
        mine = self.x[self.half(at.core, p)]
        self.sum1[p] = mine + self.got1[p] if at.cores > 1 else mine
        for o in range(1, at.chips):
            chip = lax.rem(at.chip + o, at.chips)
            self.send((2, p), self.sum1.at[p, self.piece(chip)], self.got2.at[p, o - 1], self.s2.at[p, 0, o - 1], self.r2.at[p, 0, o - 1],
                      at.at(at.core, chip, at.layer))

    def layers(self, p):
        at = self.place
        self.arrived((2, p))
        total = self.sum1[p, self.piece(at.chip)]
        for o in range(1, at.chips):
            total = total + self.got2[p, o - 1]
        self.sums[p, at.layer] = total
        for o in range(1, at.layers):
            layer = lax.rem(at.layer + o, at.layers)
            self.send((3, p), self.sums.at[p, at.layer], self.sums.at[p, at.layer], self.s3.at[p, o - 1], self.r3.at[p, o - 1],
                      at.at(at.core, at.chip, layer))

    def spread(self, p):
        at = self.place
        self.arrived((3, p))
        total = self.sums[p, 0]
        for layer in range(1, at.layers):
            total = total + self.sums[p, layer]
        rows, lanes = self.half(at.core, p)
        block = (pl.ds(pl.multiple_of(p * self.h + at.chip * self.q, 8), self.q), lanes)
        self.out[block] = total * self.scale
        for o in range(1, at.chips):
            chip = lax.rem(at.chip + o, at.chips)
            self.send((4, p), self.out.at[block], self.out.at[block], self.s2.at[p, 1, o - 1], self.r2.at[p, 1, o - 1],
                      at.at(at.core, chip, at.layer))

    def share(self, p):
        at = self.place
        self.arrived((4, p))
        if at.cores > 1:
            half = self.half(at.core, p)
            self.send((5, p), self.out.at[half], self.out.at[half], self.s1.at[p, 1], self.r1.at[p, 1],
                      at.at(1 - at.core, at.chip, at.layer))

    def run(self, step):
        for p in range(self.parts):
            step(p)

    def finish(self):
        for p in range(self.parts):
            self.arrived((5, p))

    def drain(self):
        for copy in self.started:
            copy.wait_send()


def gather_kernel(n_pts, n_hrs, widths, parts, n_points, fields_ref, probes_ref, sk_hbm, w_ref, cross_ref, *scratch):
    n = n_pts * n_hrs
    m = len(widths)
    panels, scratch = scratch[:m], scratch[m:]
    flat, part, gram, summed, sk, own_sem, send_sem, recv_sem, sk_sem, *scratch = scratch
    place = Place(n_pts, n_hrs)
    me = place.pts * n_hrs + place.hrs
    rows = fields_ref.shape[0]
    local = sum(widths)
    k, hours = part.shape

    def split_id(o):
        t = lax.rem(me + o, n)
        return t, t // n_hrs, lax.rem(t, n_hrs)

    barrier = pltpu.get_barrier_semaphore()

    @pl.loop(1, n)
    def _(o):
        _, tp, th = split_id(o)
        pl.semaphore_signal(barrier, inc=1, device_id=(tp, th), device_id_type=MESH)

    pl.semaphore_wait(barrier, n - 1)

    starts = [sum(widths[:c]) for c in range(m)]

    def source(t, c):
        return fields_ref.at[:, pl.ds(pl.multiple_of(t * local + starts[c], 128), widths[c])]

    owns = []
    for c in range(m):
        @pl.loop(1, n)
        def _(o):
            t, tp, th = split_id(o)
            pltpu.make_async_remote_copy(
                src_ref=source(t, c), dst_ref=panels[c].at[me], send_sem=send_sem.at[c], recv_sem=recv_sem.at[c],
                device_id=(tp, th), device_id_type=MESH,
            ).start()

        own = pltpu.make_async_copy(source(me, c), panels[c].at[me], own_sem.at[c])
        own.start()
        owns.append(own)

    grams = AllReduce(place, gram, summed, parts, 1.0 / n_points, scratch[:10])
    crosses = AllReduce(place, part, cross_ref, parts, 1.0 / n_points, scratch[10:])
    if gram.shape[0] > k // 2 + k // 4:
        gram[k // 2 + k // 4:, :] = jnp.zeros((gram.shape[0] - k // 2 - k // 4, k), jnp.float32)
    stores = []
    for c in range(m):
        owns[c].wait()
        most = panels[c].at[pl.ds(0, n - 1)]
        pltpu.make_async_copy(most, most, recv_sem.at[c]).wait()
        width = widths[c]
        cols = pl.ds(starts[c], width)
        if rows % 8 == 0:
            block = panels[c][...].reshape(n * rows, width)
        else:
            for d in range(n):
                flat[d * rows:(d + 1) * rows, :width] = panels[c][d]
            block = flat[:, :width]
        sketch = mm(probes_ref[...], block, ((1,), (0,)))
        sk[:, cols] = sketch
        pack(mm(sketch, sketch, ((1,), (1,))), gram, c == 0)
        if c == m - 1:
            grams.run(grams.cores)
        term = mm(sketch, block, ((1,), (1,)))
        part[...] = term if c == 0 else part[...] + term
        stores.append(pltpu.make_async_copy(sk.at[:, cols], sk_hbm.at[:, cols], sk_sem.at[c]))
        stores[-1].start()
    crosses.run(crosses.cores)
    grams.run(grams.chips)
    crosses.run(crosses.chips)
    grams.run(grams.layers)
    crosses.run(crosses.layers)
    grams.run(grams.spread)
    grams.run(grams.share)
    grams.finish()
    todo = {POINTS[p]: functools.partial(step, p % parts) for p, step in enumerate([crosses.spread] * parts + [crosses.share] * parts)}

    def between(block, panel):
        if (block, panel) in todo:
            todo[block, panel]()

    factor(summed, w_ref, between)
    crosses.finish()
    grams.drain()
    crosses.drain()
    for store in stores:
        store.wait()
    for c in range(m):
        most = panels[c].at[pl.ds(0, n - 1)]
        pltpu.make_async_copy(most, most, send_sem.at[c]).wait()


def gather(fields, probes, n_pts, n_hrs):
    k, hours = probes.shape
    rows, n_points = fields.shape
    n = n_pts * n_hrs
    local = n_points // n
    widths = pieces(local)
    m = len(widths)
    cores, low, chips, layers = split(n_pts, n_hrs)
    parts = 2 if k % (2 * chips * 8) == 0 else 1
    gram_rows = packed(k, chips, parts)
    v = pl.BlockSpec(memory_space=pltpu.VMEM)
    hbm = pl.BlockSpec(memory_space=pl.ANY)
    dma = pltpu.SemaphoreType.DMA
    f32 = jnp.float32
    return pl.pallas_call(
        functools.partial(gather_kernel, n_pts, n_hrs, widths, parts, n_points),
        out_shape=(
            jax.ShapeDtypeStruct((k, local), f32), jax.ShapeDtypeStruct((k, k), f32), jax.ShapeDtypeStruct((k, hours), f32),
        ),
        in_specs=[hbm, v],
        out_specs=(hbm, v, v),
        scratch_shapes=[
            *(pltpu.VMEM((n, rows, width), f32) for width in widths),
            pltpu.VMEM((hours, max(widths)) if rows % 8 else (8, 128), f32),
            pltpu.VMEM((k, hours), f32),
            pltpu.VMEM((gram_rows, k), f32),
            pltpu.VMEM((gram_rows, k), f32),
            pltpu.VMEM((k, local), f32),
            dma((m,)), dma((m,)), dma((m,)), dma((m,)),
            *reduce_shapes(n_pts, n_hrs, gram_rows, k, parts),
            *reduce_shapes(n_pts, n_hrs, k, hours, parts),
        ],
        compiler_params=pltpu.CompilerParams(collective_id=1, has_side_effects=True),
        name="gather",
    )(fields, probes)


def pieces(local):
    if local % 128 or local < 1024:
        return (local,)
    last = 128
    big = 512
    rest = local - last
    widths = []
    while rest > big:
        widths.append(big)
        rest -= big
    return (*widths, rest, last)


def on_device(fields, probes):
    n_pts = lax.axis_size("pts")
    n_hrs = lax.axis_size("hrs")
    sketched, w, cross = gather(fields, probes, n_pts, n_hrs)
    return finish(w, cross, sketched)


def solution(mesh):
    return jax.shard_map(
        on_device,
        mesh=mesh,
        in_specs=(P(("pts", "hrs"), None), P()),
        out_specs=(P(None, ("pts", "hrs")), P()),
        check_vma=False,
    )
```

```python
import functools

import jax
import jax.numpy as jnp
from jax import lax
from jax.experimental import pallas as pl
from jax.experimental.pallas import tpu as pltpu
from jax.sharding import PartitionSpec as P

HI = lax.Precision.HIGHEST
MESH = pl.DeviceIdType.MESH
VMEM_LIMIT = 24 * 2 ** 20
POINTS = ((0, 0), (0, 6), (1, 2), (1, 13))


def mm(a, b, dims):
    return lax.dot_general(a, b, (dims, ((), ())), precision=HI, preferred_element_type=jnp.float32)


def invert_block(block, between=None):
    b = block.shape[0]
    n = b // 8
    shape = (8, b)
    srow = lax.broadcasted_iota(jnp.int32, shape, 0)
    lane = lax.broadcasted_iota(jnp.int32, shape, 1)
    strips = [block[8 * s:8 * s + 8] for s in range(n)]
    diag = sum(jnp.where(lane == srow + 8 * s, strips[s], 0.0) for s in range(n))
    diag = jnp.broadcast_to(jnp.sum(diag, axis=0, keepdims=True), shape)
    col = 1.0 / diag
    root = lax.rsqrt(diag)
    strips = [strip * col for strip in strips]
    outs = [jnp.zeros(shape, jnp.float32)] * n

    def row_of(x, r):
        return jnp.broadcast_to(x[r:r + 1], shape)

    def spread(x, c, apart=True):
        x = jnp.broadcast_to(x[:, c:c + 1], shape)
        return jnp.maximum(x, -3e38) if apart else x

    for s0 in range(n):
        j = 8 * s0
        if between is not None:
            between(s0)
        panel = {s: [spread(strips[s], j + c, s == s0) for c in range(8)] for s in range(s0, n)}
        roots = [spread(root, j + c) for c in range(8)]
        inside = (lane >= j) & (lane < j + 8)
        for s in range(s0, n):
            unit = jnp.where(lane == srow + j, 1.0, 0.0) if s == s0 else 0.0
            strips[s] = jnp.where(inside, unit, strips[s])
        head = panel[s0]
        for p in range(0, 8, 2):
            a, b12 = row_of(head[p], p), row_of(head[p + 1], p)
            b21, c = row_of(head[p], p + 1), row_of(head[p + 1], p + 1)
            det = a * c - b12 * b21
            inv = 1.0 / det
            inva = 1.0 / a
            row1, row2 = row_of(strips[s0], p), row_of(strips[s0], p + 1)
            w1 = row1 * (lax.rsqrt(a) * roots[p])
            w2 = (row2 - (b21 * inva) * row1) * (lax.rsqrt(det * inva) * roots[p + 1])
            outs[s0] = jnp.where(srow == p, w1, jnp.where(srow == p + 1, w2, outs[s0]))
            v1, v2 = (c * row1 - b12 * row2) * inv, (a * row2 - b21 * row1) * inv
            y = {}
            for q in range(p + 2, 8):
                e1, e2 = row_of(head[q], p), row_of(head[q], p + 1)
                y[q] = (c * e1 - b12 * e2, a * e2 - b21 * e1)
            z = {q: (y[q][0] * inv, y[q][1] * inv) for q in y}
            for s in range(s0 if p < 6 else s0 + 1, n):
                f = panel[s]
                for q in range(p + 2, 8):
                    if s < s0 + 2:
                        f[q] = f[q] - (f[p] * y[q][0] + f[p + 1] * y[q][1]) * inv
                    else:
                        f[q] = f[q] - f[p] * z[q][0] - f[p + 1] * z[q][1]
                strips[s] = strips[s] - f[p] * v1 - f[p + 1] * v2
    return jnp.concatenate([jnp.where(lane <= srow + 8 * s, outs[s], 0.0) for s in range(n)], axis=0)


def packed(k, chips, parts):
    step = 8 * chips * parts
    return -(-(k // 2 + k // 4) // step) * step


def pack(g, gram, first):
    k = gram.shape[1]
    h, q = k // 2, k // 4
    for rows, cols, block in (
        (slice(0, h), slice(0, h), g[:h, :h]),
        (slice(0, h), slice(h, k), g[h:, h:]),
        (slice(h, h + q), slice(0, h), g[h:h + q, :h]),
        (slice(h, h + q), slice(h, k), g[h + q:, :h]),
    ):
        gram[rows, cols] = block if first else gram[rows, cols] + block


def factor(gram, w, between):
    k = w.shape[0]
    h, q = k // 2, k // 4
    top = invert_block(gram[:h, :h], functools.partial(between, 0))
    w[:h, :h] = top
    w[:h, h:] = jnp.zeros((h, k - h), jnp.float32)
    below = jnp.concatenate([gram[h:h + q, :h], gram[h:h + q, h:]], axis=0)
    side = mm(below, top, ((1,), (1,)))
    rest = gram[:h, h:] - mm(side, side, ((1,), (1,)))
    w[h:, :h] = mm(side, top, ((1,), (0,)))
    last = invert_block(rest, functools.partial(between, 1))
    w[h:, h:] = last
    w[h:, :h] = -mm(last, w[h:, :h], ((1,), (0,)))


def apply_kernel(w, cross, sk, basis, coeffs, y, z, sem):
    n = sk.shape[1]
    step = 512
    z[...] = mm(w[...], cross[...], ((1,), (0,)))
    stores = [pltpu.make_async_copy(z, coeffs, sem.at[0])]
    stores[0].start()
    for t in range(0, n, step):
        y[:, t:t + step] = mm(w[...], sk[:, t:t + step], ((1,), (0,)))
        stores.append(pltpu.make_async_copy(y.at[:, t:t + step], basis.at[:, t:t + step], sem.at[len(stores)]))
        stores[-1].start()
    for store in stores:
        store.wait()


def finish(w, cross, sk):
    v = pl.BlockSpec(memory_space=pltpu.VMEM)
    hbm = pl.BlockSpec(memory_space=pl.ANY)
    f32 = jnp.float32
    return pl.pallas_call(
        apply_kernel,
        out_shape=(jax.ShapeDtypeStruct(sk.shape, f32), jax.ShapeDtypeStruct(cross.shape, f32)),
        in_specs=[v, v, v],
        out_specs=(hbm, hbm),
        scratch_shapes=[
            pltpu.VMEM(sk.shape, f32), pltpu.VMEM(cross.shape, f32), pltpu.SemaphoreType.DMA((1 - -sk.shape[1] // 512,)),
        ],
        compiler_params=pltpu.CompilerParams(vmem_limit_bytes=VMEM_LIMIT),
        name="apply",
    )(w, cross, sk)


class Place:
    def __init__(self, n_pts, n_hrs):
        self.pts, self.hrs = lax.axis_index("pts"), lax.axis_index("hrs")
        self.n_pts, self.n_hrs = n_pts, n_hrs
        self.cores, self.low, self.chips, self.layers = split(n_pts, n_hrs)
        self.core = lax.rem(self.hrs, self.cores)
        self.layer = self.pts // self.low
        self.chip = (self.hrs // self.cores) * self.low + lax.rem(self.pts, self.low)

    def at(self, core, chip, layer):
        return (layer * self.low + lax.rem(chip, self.low), (chip // self.low) * self.cores + core)


def split(n_pts, n_hrs):
    cores = 2 if n_hrs % 2 == 0 else 1
    low = 1
    while n_pts % (low * 2) == 0 and low * 2 * low * 2 <= n_pts:
        low *= 2
    return cores, low, (n_hrs // cores) * low, n_pts // low


def reduce_shapes(n_pts, n_hrs, rows, width, parts):
    cores, low, chips, layers = split(n_pts, n_hrs)
    lanes = width // cores
    h = rows // parts
    q = h // chips
    f32 = jnp.float32
    dma = pltpu.SemaphoreType.DMA
    return [
        pltpu.VMEM((parts, h, lanes), f32),
        pltpu.VMEM((parts, h, lanes), f32),
        pltpu.VMEM((parts, max(chips - 1, 1), q, lanes), f32),
        pltpu.VMEM((parts, layers, q, lanes), f32),
        dma((parts, 2)), dma((parts, 2)),
        dma((parts, 2, max(chips - 1, 1))), dma((parts, 2, max(chips - 1, 1))),
        dma((parts, max(layers - 1, 1))), dma((parts, max(layers - 1, 1))),
    ]


class AllReduce:
    def __init__(self, place, x, out, parts, scale, scratch):
        self.place, self.x, self.out, self.parts, self.scale = place, x, out, parts, scale
        self.got1, self.sum1, self.got2, self.sums, self.s1, self.r1, self.s2, self.r2, self.s3, self.r3 = scratch
        self.h, self.lanes = self.got1.shape[1], self.got1.shape[2]
        self.q = self.sums.shape[2]
        self.started = []
        self.copies = {}

    def send(self, key, src, dst, ss, rs, device):
        copy = pltpu.make_async_remote_copy(
            src_ref=src, dst_ref=dst, send_sem=ss, recv_sem=rs, device_id=device, device_id_type=MESH)
        copy.start()
        self.started.append(copy)
        self.copies.setdefault(key, []).append(copy)

    def arrived(self, key):
        for copy in self.copies.get(key, ()):
            copy.wait_recv()

    def half(self, core, p):
        return pl.ds(p * self.h, self.h), pl.ds(pl.multiple_of(core * self.lanes, 128), self.lanes)

    def piece(self, chip):
        return pl.ds(pl.multiple_of(chip * self.q, 8), self.q)

    def cores(self, p):
        at = self.place
        if at.cores > 1:
            other = 1 - at.core
            self.send((1, p), self.x.at[self.half(other, p)], self.got1.at[p], self.s1.at[p, 0], self.r1.at[p, 0],
                      at.at(other, at.chip, at.layer))

    def chips(self, p):
        at = self.place
        self.arrived((1, p))
        mine = self.x[self.half(at.core, p)]
        self.sum1[p] = mine + self.got1[p] if at.cores > 1 else mine
        for o in range(1, at.chips):
            chip = lax.rem(at.chip + o, at.chips)
            self.send((2, p), self.sum1.at[p, self.piece(chip)], self.got2.at[p, o - 1], self.s2.at[p, 0, o - 1], self.r2.at[p, 0, o - 1],
                      at.at(at.core, chip, at.layer))

    def layers(self, p):
        at = self.place
        self.arrived((2, p))
        total = self.sum1[p, self.piece(at.chip)]
        for o in range(1, at.chips):
            total = total + self.got2[p, o - 1]
        self.sums[p, at.layer] = total
        for o in range(1, at.layers):
            layer = lax.rem(at.layer + o, at.layers)
            self.send((3, p), self.sums.at[p, at.layer], self.sums.at[p, at.layer], self.s3.at[p, o - 1], self.r3.at[p, o - 1],
                      at.at(at.core, at.chip, layer))

    def spread(self, p):
        at = self.place
        self.arrived((3, p))
        total = self.sums[p, 0]
        for layer in range(1, at.layers):
            total = total + self.sums[p, layer]
        rows, lanes = self.half(at.core, p)
        block = (pl.ds(pl.multiple_of(p * self.h + at.chip * self.q, 8), self.q), lanes)
        self.out[block] = total * self.scale
        for o in range(1, at.chips):
            chip = lax.rem(at.chip + o, at.chips)
            self.send((4, p), self.out.at[block], self.out.at[block], self.s2.at[p, 1, o - 1], self.r2.at[p, 1, o - 1],
                      at.at(at.core, chip, at.layer))

    def share(self, p):
        at = self.place
        self.arrived((4, p))
        if at.cores > 1:
            half = self.half(at.core, p)
            self.send((5, p), self.out.at[half], self.out.at[half], self.s1.at[p, 1], self.r1.at[p, 1],
                      at.at(1 - at.core, at.chip, at.layer))

    def run(self, step):
        for p in range(self.parts):
            step(p)

    def finish(self):
        for p in range(self.parts):
            self.arrived((5, p))

    def drain(self):
        for copy in self.started:
            copy.wait_send()


def gather_kernel(n_pts, n_hrs, widths, parts, n_points, fields_ref, probes_hbm, sk_hbm, w_ref, cross_ref, *scratch):
    n = n_pts * n_hrs
    m = len(widths)
    panels, scratch = scratch[:m], scratch[m:]
    flat, probes_ref, part, gram, summed, sk, probes_sem, own_sem, send_sem, recv_sem, sk_sem, *scratch = scratch
    place = Place(n_pts, n_hrs)
    me = place.pts * n_hrs + place.hrs
    rows = fields_ref.shape[0]
    local = sum(widths)
    k, hours = part.shape

    def split_id(o):
        t = lax.rem(me + o, n)
        return t, t // n_hrs, lax.rem(t, n_hrs)

    probes_load = pltpu.make_async_copy(probes_hbm, probes_ref, probes_sem)
    probes_load.start()
    barrier = pltpu.get_barrier_semaphore()

    @pl.loop(1, n)
    def _(o):
        _, tp, th = split_id(o)
        pl.semaphore_signal(barrier, inc=1, device_id=(tp, th), device_id_type=MESH)

    pl.semaphore_wait(barrier, n - 1)

    starts = [sum(widths[:c]) for c in range(m)]

    def source(t, c):
        return fields_ref.at[:, pl.ds(pl.multiple_of(t * local + starts[c], 128), widths[c])]

    owns = []
    for c in range(m):
        @pl.loop(1, n)
        def _(o):
            t, tp, th = split_id(o)
            pltpu.make_async_remote_copy(
                src_ref=source(t, c), dst_ref=panels[c].at[me], send_sem=send_sem.at[c], recv_sem=recv_sem.at[c],
                device_id=(tp, th), device_id_type=MESH,
            ).start()

        own = pltpu.make_async_copy(source(me, c), panels[c].at[me], own_sem.at[c])
        own.start()
        owns.append(own)

    grams = AllReduce(place, gram, summed, parts, 1.0 / n_points, scratch[:10])
    crosses = AllReduce(place, part, cross_ref, parts, 1.0 / n_points, scratch[10:])
    if gram.shape[0] > k // 2 + k // 4:
        gram[k // 2 + k // 4:, :] = jnp.zeros((gram.shape[0] - k // 2 - k // 4, k), jnp.float32)
    stores = []
    probes_load.wait()
    for c in range(m):
        owns[c].wait()
        most = panels[c].at[pl.ds(0, n - 1)]
        pltpu.make_async_copy(most, most, recv_sem.at[c]).wait()
        width = widths[c]
        cols = pl.ds(starts[c], width)
        if rows % 8 == 0:
            block = panels[c][...].reshape(n * rows, width)
        else:
            for d in range(n):
                flat[d * rows:(d + 1) * rows, :width] = panels[c][d]
            block = flat[:, :width]
        sketch = mm(probes_ref[...], block, ((1,), (0,)))
        sk[:, cols] = sketch
        pack(mm(sketch, sketch, ((1,), (1,))), gram, c == 0)
        if c == m - 1:
            grams.run(grams.cores)
        term = mm(sketch, block, ((1,), (1,)))
        part[...] = term if c == 0 else part[...] + term
        stores.append(pltpu.make_async_copy(sk.at[:, cols], sk_hbm.at[:, cols], sk_sem.at[c]))
        stores[-1].start()
    crosses.run(crosses.cores)
    grams.run(grams.chips)
    crosses.run(crosses.chips)
    grams.run(grams.layers)
    crosses.run(crosses.layers)
    grams.run(grams.spread)
    grams.run(grams.share)
    grams.finish()
    todo = {POINTS[p]: functools.partial(step, p % parts) for p, step in enumerate([crosses.spread] * parts + [crosses.share] * parts)}

    def between(block, panel):
        if (block, panel) in todo:
            todo[block, panel]()

    factor(summed, w_ref, between)
    crosses.finish()
    grams.drain()
    crosses.drain()
    for store in stores:
        store.wait()
    for c in range(m):
        most = panels[c].at[pl.ds(0, n - 1)]
        pltpu.make_async_copy(most, most, send_sem.at[c]).wait()


def gather(fields, probes, n_pts, n_hrs):
    k, hours = probes.shape
    rows, n_points = fields.shape
    n = n_pts * n_hrs
    local = n_points // n
    widths = pieces(local)
    m = len(widths)
    cores, low, chips, layers = split(n_pts, n_hrs)
    parts = 2 if k % (2 * chips * 8) == 0 else 1
    gram_rows = packed(k, chips, parts)
    v = pl.BlockSpec(memory_space=pltpu.VMEM)
    hbm = pl.BlockSpec(memory_space=pl.ANY)
    far = pl.BlockSpec(memory_space=pltpu.HBM)
    dma = pltpu.SemaphoreType.DMA
    f32 = jnp.float32
    return pl.pallas_call(
        functools.partial(gather_kernel, n_pts, n_hrs, widths, parts, n_points),
        out_shape=(
            jax.ShapeDtypeStruct((k, local), f32), jax.ShapeDtypeStruct((k, k), f32), jax.ShapeDtypeStruct((k, hours), f32),
        ),
        in_specs=[far, far],
        out_specs=(hbm, v, v),
        scratch_shapes=[
            *(pltpu.VMEM((n, rows, width), f32) for width in widths),
            pltpu.VMEM((hours, max(widths)) if rows % 8 else (8, 128), f32),
            pltpu.VMEM((k, hours), f32),
            pltpu.VMEM((k, hours), f32),
            pltpu.VMEM((gram_rows, k), f32),
            pltpu.VMEM((gram_rows, k), f32),
            pltpu.VMEM((k, local), f32),
            dma(()), dma((m,)), dma((m,)), dma((m,)), dma((m,)),
            *reduce_shapes(n_pts, n_hrs, gram_rows, k, parts),
            *reduce_shapes(n_pts, n_hrs, k, hours, parts),
        ],
        compiler_params=pltpu.CompilerParams(collective_id=1, has_side_effects=True, vmem_limit_bytes=VMEM_LIMIT),
        name="gather",
    )(fields, probes)


def pieces(local):
    if local % 128 or local < 1024:
        return (local,)
    last = 128
    big = 512
    rest = local - last
    widths = []
    while rest > big:
        widths.append(big)
        rest -= big
    return (*widths, rest, last)


def on_device(fields, probes):
    n_pts = lax.axis_size("pts")
    n_hrs = lax.axis_size("hrs")
    sketched, w, cross = gather(pltpu.with_memory_space_constraint(fields, pltpu.HBM), pltpu.with_memory_space_constraint(probes, pltpu.HBM), n_pts, n_hrs)
    return finish(w, cross, sketched)


def solution(mesh):
    return jax.shard_map(
        on_device,
        mesh=mesh,
        in_specs=(P(("pts", "hrs"), None), P()),
        out_specs=(P(None, ("pts", "hrs")), P()),
        check_vma=False,
    )
```

```python
import functools

import jax
import jax.numpy as jnp
from jax import lax
from jax.experimental import pallas as pl
from jax.experimental.pallas import tpu as pltpu
from jax.sharding import PartitionSpec as P

HI = lax.Precision.HIGHEST
YP = lax.Precision.HIGH
MESH = pl.DeviceIdType.MESH
VMEM_LIMIT = 24 * 2 ** 20
POINTS = ((0, 0), (0, 5), (1, 2), (1, 12))


def mm(a, b, dims, precision=HI):
    return lax.dot_general(a, b, (dims, ((), ())), precision=precision, preferred_element_type=jnp.float32)


def invert_block(block, between=None):
    b = block.shape[0]
    n = b // 8
    shape = (8, b)
    srow = lax.broadcasted_iota(jnp.int32, shape, 0)
    lane = lax.broadcasted_iota(jnp.int32, shape, 1)
    strips = [block[8 * s:8 * s + 8] for s in range(n)]
    diag = sum(jnp.where(lane == srow + 8 * s, strips[s], 0.0) for s in range(n))
    diag = jnp.broadcast_to(jnp.sum(diag, axis=0, keepdims=True), shape)
    col = 1.0 / diag
    root = lax.rsqrt(diag)
    strips = [strip * col for strip in strips]
    outs = [jnp.zeros(shape, jnp.float32)] * n

    def row_of(x, r):
        return jnp.broadcast_to(x[r:r + 1], shape)

    def spread(x, c, apart=True):
        x = jnp.broadcast_to(x[:, c:c + 1], shape)
        return jnp.maximum(x, -3e38) if apart else x

    for s0 in range(n):
        j = 8 * s0
        if between is not None:
            between(s0)
        panel = {s: [spread(strips[s], j + c, s == s0) for c in range(8)] for s in range(s0, n)}
        roots = [spread(root, j + c) for c in range(8)]
        inside = (lane >= j) & (lane < j + 8)
        for s in range(s0, n):
            unit = jnp.where(lane == srow + j, 1.0, 0.0) if s == s0 else 0.0
            strips[s] = jnp.where(inside, unit, strips[s])
        head = panel[s0]
        for p in range(0, 8, 2):
            a, b12 = row_of(head[p], p), row_of(head[p + 1], p)
            b21, c = row_of(head[p], p + 1), row_of(head[p + 1], p + 1)
            det = a * c - b12 * b21
            inv = 1.0 / det
            inva = 1.0 / a
            row1, row2 = row_of(strips[s0], p), row_of(strips[s0], p + 1)
            w1 = row1 * (lax.rsqrt(a) * roots[p])
            w2 = (row2 - (b21 * inva) * row1) * (lax.rsqrt(det * inva) * roots[p + 1])
            outs[s0] = jnp.where(srow == p, w1, jnp.where(srow == p + 1, w2, outs[s0]))
            v1, v2 = (c * row1 - b12 * row2) * inv, (a * row2 - b21 * row1) * inv
            y = {}
            for q in range(p + 2, 8):
                e1, e2 = row_of(head[q], p), row_of(head[q], p + 1)
                y[q] = (c * e1 - b12 * e2, a * e2 - b21 * e1)
            z = {q: (y[q][0] * inv, y[q][1] * inv) for q in y}
            for s in range(s0 if p < 6 else s0 + 1, n):
                f = panel[s]
                for q in range(p + 2, 8):
                    if s < s0 + 2:
                        f[q] = f[q] - (f[p] * y[q][0] + f[p + 1] * y[q][1]) * inv
                    else:
                        f[q] = f[q] - f[p] * z[q][0] - f[p + 1] * z[q][1]
                strips[s] = strips[s] - f[p] * v1 - f[p + 1] * v2
    return jnp.concatenate([jnp.where(lane <= srow + 8 * s, outs[s], 0.0) for s in range(n)], axis=0)


def packed(k, chips, parts):
    step = 8 * chips * parts
    return -(-(k // 2 + k // 4) // step) * step


def pack(g, gram, first):
    k = gram.shape[1]
    h, q = k // 2, k // 4
    for rows, cols, block in (
        (slice(0, h), slice(0, h), g[:h, :h]),
        (slice(0, h), slice(h, k), g[h:, h:]),
        (slice(h, h + q), slice(0, h), g[h:h + q, :h]),
        (slice(h, h + q), slice(h, k), g[h + q:, :h]),
    ):
        gram[rows, cols] = block if first else gram[rows, cols] + block


def factor(gram, w, between):
    k = w.shape[0]
    h, q = k // 2, k // 4
    top = invert_block(gram[:h, :h], functools.partial(between, 0))
    w[:h, :h] = top
    w[:h, h:] = jnp.zeros((h, k - h), jnp.float32)
    below = jnp.concatenate([gram[h:h + q, :h], gram[h:h + q, h:]], axis=0)
    side = mm(below, top, ((1,), (1,)))
    rest = gram[:h, h:] - mm(side, side, ((1,), (1,)))
    w[h:, :h] = mm(side, top, ((1,), (0,)))
    last = invert_block(rest, functools.partial(between, 1))
    w[h:, h:] = last
    w[h:, :h] = -mm(last, w[h:, :h], ((1,), (0,)))


def output_kernel(w, cross, y, basis, coeffs, z, sem):
    first = pltpu.make_async_copy(y, basis, sem.at[0])
    first.start()
    z[...] = mm(w[...], cross[...], ((1,), (0,)))
    second = pltpu.make_async_copy(z, coeffs, sem.at[1])
    second.start()
    first.wait()
    second.wait()


def finish(w, cross, y):
    v = pl.BlockSpec(memory_space=pltpu.VMEM)
    hbm = pl.BlockSpec(memory_space=pl.ANY)
    f32 = jnp.float32
    return pl.pallas_call(
        output_kernel,
        out_shape=(jax.ShapeDtypeStruct(y.shape, f32), jax.ShapeDtypeStruct(cross.shape, f32)),
        in_specs=[v, v, v],
        out_specs=(hbm, hbm),
        scratch_shapes=[pltpu.VMEM(cross.shape, f32), pltpu.SemaphoreType.DMA((2,))],
        compiler_params=pltpu.CompilerParams(vmem_limit_bytes=VMEM_LIMIT),
        name="output",
    )(w, cross, y)


class Place:
    def __init__(self, n_pts, n_hrs):
        self.pts, self.hrs = lax.axis_index("pts"), lax.axis_index("hrs")
        self.n_pts, self.n_hrs = n_pts, n_hrs
        self.cores, self.low, self.chips, self.layers = split(n_pts, n_hrs)
        self.core = lax.rem(self.hrs, self.cores)
        self.layer = self.pts // self.low
        self.chip = (self.hrs // self.cores) * self.low + lax.rem(self.pts, self.low)

    def at(self, core, chip, layer):
        return (layer * self.low + lax.rem(chip, self.low), (chip // self.low) * self.cores + core)


def split(n_pts, n_hrs):
    cores = 2 if n_hrs % 2 == 0 else 1
    low = 1
    while n_pts % (low * 2) == 0 and low * 2 * low * 2 <= n_pts:
        low *= 2
    return cores, low, (n_hrs // cores) * low, n_pts // low


def reduce_shapes(n_pts, n_hrs, rows, width, parts):
    cores, low, chips, layers = split(n_pts, n_hrs)
    lanes = width // cores
    h = rows // parts
    q = h // chips
    f32 = jnp.float32
    dma = pltpu.SemaphoreType.DMA
    return [
        pltpu.VMEM((parts, h, lanes), f32),
        pltpu.VMEM((parts, h, lanes), f32),
        pltpu.VMEM((parts, max(chips - 1, 1), q, lanes), f32),
        pltpu.VMEM((parts, layers, q, lanes), f32),
        dma((parts, 2)), dma((parts, 2)),
        dma((parts, 2, max(chips - 1, 1))), dma((parts, 2, max(chips - 1, 1))),
        dma((parts, max(layers - 1, 1))), dma((parts, max(layers - 1, 1))),
    ]


class AllReduce:
    def __init__(self, place, x, out, parts, scale, scratch):
        self.place, self.x, self.out, self.parts, self.scale = place, x, out, parts, scale
        self.got1, self.sum1, self.got2, self.sums, self.s1, self.r1, self.s2, self.r2, self.s3, self.r3 = scratch
        self.h, self.lanes = self.got1.shape[1], self.got1.shape[2]
        self.q = self.sums.shape[2]
        self.started = []
        self.copies = {}

    def send(self, key, src, dst, ss, rs, device):
        copy = pltpu.make_async_remote_copy(
            src_ref=src, dst_ref=dst, send_sem=ss, recv_sem=rs, device_id=device, device_id_type=MESH)
        copy.start()
        self.started.append(copy)
        self.copies.setdefault(key, []).append(copy)

    def arrived(self, key):
        for copy in self.copies.get(key, ()):
            copy.wait_recv()

    def half(self, core, p):
        return pl.ds(p * self.h, self.h), pl.ds(pl.multiple_of(core * self.lanes, 128), self.lanes)

    def piece(self, chip):
        return pl.ds(pl.multiple_of(chip * self.q, 8), self.q)

    def cores(self, p):
        at = self.place
        if at.cores > 1:
            other = 1 - at.core
            self.send((1, p), self.x.at[self.half(other, p)], self.got1.at[p], self.s1.at[p, 0], self.r1.at[p, 0],
                      at.at(other, at.chip, at.layer))

    def chips(self, p):
        at = self.place
        self.arrived((1, p))
        mine = self.x[self.half(at.core, p)]
        self.sum1[p] = mine + self.got1[p] if at.cores > 1 else mine
        for o in range(1, at.chips):
            chip = lax.rem(at.chip + o, at.chips)
            self.send((2, p), self.sum1.at[p, self.piece(chip)], self.got2.at[p, o - 1], self.s2.at[p, 0, o - 1], self.r2.at[p, 0, o - 1],
                      at.at(at.core, chip, at.layer))

    def layers(self, p):
        at = self.place
        self.arrived((2, p))
        total = self.sum1[p, self.piece(at.chip)]
        for o in range(1, at.chips):
            total = total + self.got2[p, o - 1]
        self.sums[p, at.layer] = total
        for o in range(1, at.layers):
            layer = lax.rem(at.layer + o, at.layers)
            self.send((3, p), self.sums.at[p, at.layer], self.sums.at[p, at.layer], self.s3.at[p, o - 1], self.r3.at[p, o - 1],
                      at.at(at.core, at.chip, layer))

    def spread(self, p):
        at = self.place
        self.arrived((3, p))
        total = self.sums[p, 0]
        for layer in range(1, at.layers):
            total = total + self.sums[p, layer]
        rows, lanes = self.half(at.core, p)
        block = (pl.ds(pl.multiple_of(p * self.h + at.chip * self.q, 8), self.q), lanes)
        self.out[block] = total * self.scale
        for o in range(1, at.chips):
            chip = lax.rem(at.chip + o, at.chips)
            self.send((4, p), self.out.at[block], self.out.at[block], self.s2.at[p, 1, o - 1], self.r2.at[p, 1, o - 1],
                      at.at(at.core, chip, at.layer))

    def share(self, p):
        at = self.place
        self.arrived((4, p))
        if at.cores > 1:
            half = self.half(at.core, p)
            self.send((5, p), self.out.at[half], self.out.at[half], self.s1.at[p, 1], self.r1.at[p, 1],
                      at.at(1 - at.core, at.chip, at.layer))

    def run(self, step):
        for p in range(self.parts):
            step(p)

    def finish(self):
        for p in range(self.parts):
            self.arrived((5, p))

    def drain(self):
        for copy in self.started:
            copy.wait_send()


def gather_kernel(n_pts, n_hrs, widths, parts, n_points, fields_ref, probes_hbm, y_ref, w_ref, cross_ref, *scratch):
    n = n_pts * n_hrs
    m = len(widths)
    panels, scratch = scratch[:m], scratch[m:]
    flat, probes_ref, part, gram, summed, sk, probes_sem, own_sem, send_sem, recv_sem, *scratch = scratch
    place = Place(n_pts, n_hrs)
    me = place.pts * n_hrs + place.hrs
    rows = fields_ref.shape[0]
    local = sum(widths)
    k, hours = part.shape

    def split_id(o):
        t = lax.rem(me + o, n)
        return t, t // n_hrs, lax.rem(t, n_hrs)

    probes_load = pltpu.make_async_copy(probes_hbm, probes_ref, probes_sem)
    probes_load.start()
    barrier = pltpu.get_barrier_semaphore()

    @pl.loop(1, n)
    def _(o):
        _, tp, th = split_id(o)
        pl.semaphore_signal(barrier, inc=1, device_id=(tp, th), device_id_type=MESH)

    pl.semaphore_wait(barrier, n - 1)

    starts = [sum(widths[:c]) for c in range(m)]

    def source(t, c):
        return fields_ref.at[:, pl.ds(pl.multiple_of(t * local + starts[c], 128), widths[c])]

    owns = []
    for c in range(m):
        @pl.loop(1, n)
        def _(o):
            t, tp, th = split_id(o)
            pltpu.make_async_remote_copy(
                src_ref=source(t, c), dst_ref=panels[c].at[me], send_sem=send_sem.at[c], recv_sem=recv_sem.at[c],
                device_id=(tp, th), device_id_type=MESH,
            ).start()

        own = pltpu.make_async_copy(source(me, c), panels[c].at[me], own_sem.at[c])
        own.start()
        owns.append(own)

    grams = AllReduce(place, gram, summed, parts, 1.0 / n_points, scratch[:10])
    crosses = AllReduce(place, part, cross_ref, parts, 1.0 / n_points, scratch[10:])
    if gram.shape[0] > k // 2 + k // 4:
        gram[k // 2 + k // 4:, :] = jnp.zeros((gram.shape[0] - k // 2 - k // 4, k), jnp.float32)
    probes_load.wait()
    for c in range(m):
        owns[c].wait()
        most = panels[c].at[pl.ds(0, n - 1)]
        pltpu.make_async_copy(most, most, recv_sem.at[c]).wait()
        width = widths[c]
        cols = pl.ds(starts[c], width)
        if rows % 8 == 0:
            block = panels[c][...].reshape(n * rows, width)
        else:
            for d in range(n):
                flat[d * rows:(d + 1) * rows, :width] = panels[c][d]
            block = flat[:, :width]
        sketch = mm(probes_ref[...], block, ((1,), (0,)))
        sk[:, cols] = sketch
        pack(mm(sketch, sketch, ((1,), (1,))), gram, c == 0)
        if c == m - 1:
            grams.run(grams.cores)
        if c < m - 1:
            term = mm(sketch, block, ((1,), (1,)))
            part[...] = term if c == 0 else part[...] + term
        else:
            span = n // crosses.place.cores
            for own in range(crosses.place.cores):
                core = lax.rem(crosses.place.core + 1 + own, crosses.place.cores)
                lanes = pl.ds(pl.multiple_of(core * span * rows, 128), span * rows)
                if rows % 8 == 0:
                    block = panels[c][pl.ds(core * span, span)].reshape(span * rows, width)
                else:
                    block = flat[pl.ds(pl.multiple_of(core * span * rows, 8), span * rows), :width]
                term = mm(sketch, block, ((1,), (1,)))
                part[:, lanes] = term if c == 0 else part[:, lanes] + term
                if own == 0:
                    crosses.run(crosses.cores)
    grams.run(grams.chips)
    crosses.run(crosses.chips)
    grams.run(grams.layers)
    crosses.run(crosses.layers)
    grams.run(grams.spread)
    grams.run(grams.share)
    grams.finish()
    todo = {POINTS[p]: functools.partial(step, p % parts) for p, step in enumerate([crosses.spread] * parts + [crosses.share] * parts)}


    def between(block, panel):
        if (block, panel) in todo:
            todo[block, panel]()

    factor(summed, w_ref, between)
    step = 512
    for t in range(0, local, step):
        y_ref[:, t:t + step] = mm(w_ref[...], sk[:, t:t + step], ((1,), (0,)), YP)
    crosses.finish()
    grams.drain()
    crosses.drain()
    for c in range(m):
        most = panels[c].at[pl.ds(0, n - 1)]
        pltpu.make_async_copy(most, most, send_sem.at[c]).wait()


def gather(fields, probes, n_pts, n_hrs):
    k, hours = probes.shape
    rows, n_points = fields.shape
    n = n_pts * n_hrs
    local = n_points // n
    widths = pieces(local)
    m = len(widths)
    cores, low, chips, layers = split(n_pts, n_hrs)
    parts = 2 if k % (2 * chips * 8) == 0 else 1
    gram_rows = packed(k, chips, parts)
    v = pl.BlockSpec(memory_space=pltpu.VMEM)
    far = pl.BlockSpec(memory_space=pltpu.HBM)
    dma = pltpu.SemaphoreType.DMA
    f32 = jnp.float32
    return pl.pallas_call(
        functools.partial(gather_kernel, n_pts, n_hrs, widths, parts, n_points),
        out_shape=(
            jax.ShapeDtypeStruct((k, local), f32), jax.ShapeDtypeStruct((k, k), f32), jax.ShapeDtypeStruct((k, hours), f32),
        ),
        in_specs=[far, far],
        out_specs=(v, v, v),
        scratch_shapes=[
            *(pltpu.VMEM((n, rows, width), f32) for width in widths),
            pltpu.VMEM((hours, max(widths)) if rows % 8 else (8, 128), f32),
            pltpu.VMEM((k, hours), f32),
            pltpu.VMEM((k, hours), f32),
            pltpu.VMEM((gram_rows, k), f32),
            pltpu.VMEM((gram_rows, k), f32),
            pltpu.VMEM((k, local), f32),
            dma(()), dma((m,)), dma((m,)), dma((m,)),
            *reduce_shapes(n_pts, n_hrs, gram_rows, k, parts),
            *reduce_shapes(n_pts, n_hrs, k, hours, parts),
        ],
        compiler_params=pltpu.CompilerParams(collective_id=1, has_side_effects=True, vmem_limit_bytes=VMEM_LIMIT),
        name="gather",
    )(fields, probes)


def pieces(local):
    if local % 128 or local < 1024:
        return (local,)
    last = 128
    big = 512
    rest = local - last
    widths = []
    while rest > big:
        widths.append(big)
        rest -= big
    return (*widths, rest, last)


def on_device(fields, probes):
    n_pts = lax.axis_size("pts")
    n_hrs = lax.axis_size("hrs")
    y, w, cross = gather(pltpu.with_memory_space_constraint(fields, pltpu.HBM), pltpu.with_memory_space_constraint(probes, pltpu.HBM), n_pts, n_hrs)
    return finish(w, cross, y)


def solution(mesh):
    return jax.shard_map(
        on_device,
        mesh=mesh,
        in_specs=(P(("pts", "hrs"), None), P()),
        out_specs=(P(None, ("pts", "hrs")), P()),
        check_vma=False,
    )
```

```python
import functools

import jax
import jax.numpy as jnp
from jax import lax
from jax.experimental import pallas as pl
from jax.experimental.pallas import tpu as pltpu
from jax.sharding import PartitionSpec as P

HI = lax.Precision.HIGHEST
MESH = pl.DeviceIdType.MESH
VMEM_LIMIT = 24 * 2 ** 20
POINTS = ((0, 1), (0, 7), (1, 4), (1, 14))


def mm(a, b, dims):
    return lax.dot_general(a, b, (dims, ((), ())), precision=HI, preferred_element_type=jnp.float32)


def invert_block(block, between=None):
    b = block.shape[0]
    n = b // 8
    shape = (8, b)
    srow = lax.broadcasted_iota(jnp.int32, shape, 0)
    lane = lax.broadcasted_iota(jnp.int32, shape, 1)
    strips = [block[8 * s:8 * s + 8] for s in range(n)]
    diag = sum(jnp.where(lane == srow + 8 * s, strips[s], 0.0) for s in range(n))
    diag = jnp.broadcast_to(jnp.sum(diag, axis=0, keepdims=True), shape)
    col = 1.0 / diag
    root = lax.rsqrt(diag)
    strips = [strip * col for strip in strips]
    outs = [jnp.zeros(shape, jnp.float32)] * n

    def row_of(x, r):
        return jnp.broadcast_to(x[r:r + 1], shape)

    def spread(x, c, apart=True):
        x = jnp.broadcast_to(x[:, c:c + 1], shape)
        return jnp.maximum(x, -3e38) if apart else x

    for s0 in range(n):
        j = 8 * s0
        if between is not None:
            between(s0)
        panel = {s: [spread(strips[s], j + c, s == s0) for c in range(8)] for s in range(s0, n)}
        roots = [spread(root, j + c) for c in range(8)]
        inside = (lane >= j) & (lane < j + 8)
        for s in range(s0, n):
            unit = jnp.where(lane == srow + j, 1.0, 0.0) if s == s0 else 0.0
            strips[s] = jnp.where(inside, unit, strips[s])
        head = panel[s0]
        for p in range(0, 8, 2):
            a, b12 = row_of(head[p], p), row_of(head[p + 1], p)
            b21, c = row_of(head[p], p + 1), row_of(head[p + 1], p + 1)
            det = a * c - b12 * b21
            inv = 1.0 / det
            inva = 1.0 / a
            row1, row2 = row_of(strips[s0], p), row_of(strips[s0], p + 1)
            w1 = row1 * (lax.rsqrt(a) * roots[p])
            w2 = (row2 - (b21 * inva) * row1) * (lax.rsqrt(det * inva) * roots[p + 1])
            outs[s0] = jnp.where(srow == p, w1, jnp.where(srow == p + 1, w2, outs[s0]))
            v1, v2 = (c * row1 - b12 * row2) * inv, (a * row2 - b21 * row1) * inv
            y = {}
            for q in range(p + 2, 8):
                e1, e2 = row_of(head[q], p), row_of(head[q], p + 1)
                y[q] = (c * e1 - b12 * e2, a * e2 - b21 * e1)
            z = {q: (y[q][0] * inv, y[q][1] * inv) for q in y}
            for s in range(s0 if p < 6 else s0 + 1, n):
                f = panel[s]
                for q in range(p + 2, 8):
                    if s < s0 + 2:
                        f[q] = f[q] - (f[p] * y[q][0] + f[p + 1] * y[q][1]) * inv
                    else:
                        f[q] = f[q] - f[p] * z[q][0] - f[p + 1] * z[q][1]
                strips[s] = strips[s] - f[p] * v1 - f[p + 1] * v2
    return jnp.concatenate([jnp.where(lane <= srow + 8 * s, outs[s], 0.0) for s in range(n)], axis=0)


def padded(rows, chips):
    return -(-rows // (8 * chips)) * 8 * chips


def pack(g, head, rest, first):
    k = g.shape[0]
    h, q = k // 2, k // 4
    for ref, rows, cols, block in (
        (head, slice(0, q), slice(0, h), g[:q, :h]),
        (head, slice(0, q), slice(h, k), g[q:h, :h]),
        (rest, slice(0, h), slice(0, h), g[h:, h:]),
        (rest, slice(0, h), slice(h, k), g[h:, :h]),
    ):
        ref[rows, cols] = block if first else ref[rows, cols] + block


def factor(head, rest, w, between):
    k = w.shape[0]
    h, q = k // 2, k // 4
    first = jnp.concatenate([head[:q, :h], head[:q, h:]], axis=0)
    top = invert_block(first, functools.partial(between, 0))
    w[:h, :h] = top
    w[:h, h:] = jnp.zeros((h, k - h), jnp.float32)
    between(0, -1)
    side = mm(rest[:h, h:], top, ((1,), (1,)))
    second = rest[:h, :h] - mm(side, side, ((1,), (1,)))
    w[h:, :h] = mm(side, top, ((1,), (0,)))
    last = invert_block(second, functools.partial(between, 1))
    w[h:, h:] = last
    w[h:, :h] = -mm(last, w[h:, :h], ((1,), (0,)))


def output_kernel(w, cross, y, basis, coeffs, z, sem):
    first = pltpu.make_async_copy(y, basis, sem.at[0])
    first.start()
    z[...] = mm(w[...], cross[...], ((1,), (0,)))
    second = pltpu.make_async_copy(z, coeffs, sem.at[1])
    second.start()
    first.wait()
    second.wait()


def finish(w, cross, y):
    v = pl.BlockSpec(memory_space=pltpu.VMEM)
    hbm = pl.BlockSpec(memory_space=pl.ANY)
    f32 = jnp.float32
    return pl.pallas_call(
        output_kernel,
        out_shape=(jax.ShapeDtypeStruct(y.shape, f32), jax.ShapeDtypeStruct(cross.shape, f32)),
        in_specs=[v, v, v],
        out_specs=(hbm, hbm),
        scratch_shapes=[pltpu.VMEM(cross.shape, f32), pltpu.SemaphoreType.DMA((2,))],
        compiler_params=pltpu.CompilerParams(vmem_limit_bytes=VMEM_LIMIT),
        name="output",
    )(w, cross, y)


class Place:
    def __init__(self, n_pts, n_hrs):
        self.pts, self.hrs = lax.axis_index("pts"), lax.axis_index("hrs")
        self.n_pts, self.n_hrs = n_pts, n_hrs
        self.cores, self.low, self.chips, self.layers = split(n_pts, n_hrs)
        self.core = lax.rem(self.hrs, self.cores)
        self.layer = self.pts // self.low
        self.chip = (self.hrs // self.cores) * self.low + lax.rem(self.pts, self.low)

    def at(self, core, chip, layer):
        return (layer * self.low + lax.rem(chip, self.low), (chip // self.low) * self.cores + core)


def split(n_pts, n_hrs):
    cores = 2 if n_hrs % 2 == 0 else 1
    low = 1
    while n_pts % (low * 2) == 0 and low * 2 * low * 2 <= n_pts:
        low *= 2
    return cores, low, (n_hrs // cores) * low, n_pts // low


def reduce_shapes(n_pts, n_hrs, rows, width, parts):
    cores, low, chips, layers = split(n_pts, n_hrs)
    lanes = width // cores
    h = rows // parts
    q = h // chips
    f32 = jnp.float32
    dma = pltpu.SemaphoreType.DMA
    return [
        pltpu.VMEM((parts, h, lanes), f32),
        pltpu.VMEM((parts, h, lanes), f32),
        pltpu.VMEM((parts, max(chips - 1, 1), q, lanes), f32),
        pltpu.VMEM((parts, layers, q, lanes), f32),
        dma((parts, 2)), dma((parts, 2)),
        dma((parts, 2, max(chips - 1, 1))), dma((parts, 2, max(chips - 1, 1))),
        dma((parts, max(layers - 1, 1))), dma((parts, max(layers - 1, 1))),
    ]


class AllReduce:
    def __init__(self, place, x, out, parts, scale, scratch):
        self.place, self.x, self.out, self.parts, self.scale = place, x, out, parts, scale
        self.got1, self.sum1, self.got2, self.sums, self.s1, self.r1, self.s2, self.r2, self.s3, self.r3 = scratch
        self.h, self.lanes = self.got1.shape[1], self.got1.shape[2]
        self.q = self.sums.shape[2]
        self.started = []
        self.copies = {}

    def send(self, key, src, dst, ss, rs, device):
        copy = pltpu.make_async_remote_copy(
            src_ref=src, dst_ref=dst, send_sem=ss, recv_sem=rs, device_id=device, device_id_type=MESH)
        copy.start()
        self.started.append(copy)
        self.copies.setdefault(key, []).append(copy)

    def arrived(self, key):
        for copy in self.copies.get(key, ()):
            copy.wait_recv()

    def half(self, core, p):
        return pl.ds(p * self.h, self.h), pl.ds(pl.multiple_of(core * self.lanes, 128), self.lanes)

    def piece(self, chip):
        return pl.ds(pl.multiple_of(chip * self.q, 8), self.q)

    def cores(self, p):
        at = self.place
        if at.cores > 1:
            other = 1 - at.core
            self.send((1, p), self.x.at[self.half(other, p)], self.got1.at[p], self.s1.at[p, 0], self.r1.at[p, 0],
                      at.at(other, at.chip, at.layer))

    def chips(self, p):
        at = self.place
        self.arrived((1, p))
        mine = self.x[self.half(at.core, p)]
        self.sum1[p] = mine + self.got1[p] if at.cores > 1 else mine
        for o in range(1, at.chips):
            chip = lax.rem(at.chip + o, at.chips)
            self.send((2, p), self.sum1.at[p, self.piece(chip)], self.got2.at[p, o - 1], self.s2.at[p, 0, o - 1], self.r2.at[p, 0, o - 1],
                      at.at(at.core, chip, at.layer))

    def layers(self, p):
        at = self.place
        self.arrived((2, p))
        total = self.sum1[p, self.piece(at.chip)]
        for o in range(1, at.chips):
            total = total + self.got2[p, o - 1]
        self.sums[p, at.layer] = total
        for o in range(1, at.layers):
            layer = lax.rem(at.layer + o, at.layers)
            self.send((3, p), self.sums.at[p, at.layer], self.sums.at[p, at.layer], self.s3.at[p, o - 1], self.r3.at[p, o - 1],
                      at.at(at.core, at.chip, layer))

    def spread(self, p):
        at = self.place
        self.arrived((3, p))
        total = self.sums[p, 0]
        for layer in range(1, at.layers):
            total = total + self.sums[p, layer]
        rows, lanes = self.half(at.core, p)
        block = (pl.ds(pl.multiple_of(p * self.h + at.chip * self.q, 8), self.q), lanes)
        self.out[block] = total * self.scale
        for o in range(1, at.chips):
            chip = lax.rem(at.chip + o, at.chips)
            self.send((4, p), self.out.at[block], self.out.at[block], self.s2.at[p, 1, o - 1], self.r2.at[p, 1, o - 1],
                      at.at(at.core, chip, at.layer))

    def share(self, p):
        at = self.place
        self.arrived((4, p))
        if at.cores > 1:
            half = self.half(at.core, p)
            self.send((5, p), self.out.at[half], self.out.at[half], self.s1.at[p, 1], self.r1.at[p, 1],
                      at.at(1 - at.core, at.chip, at.layer))

    def run(self, step):
        for p in range(self.parts):
            step(p)

    def finish(self):
        for p in range(self.parts):
            self.arrived((5, p))

    def drain(self):
        for copy in self.started:
            copy.wait_send()


def gather_kernel(n_pts, n_hrs, widths, parts, n_points, fields_ref, probes_hbm, y_ref, w_ref, cross_ref, *scratch):
    n = n_pts * n_hrs
    m = len(widths)
    panels, scratch = scratch[:m], scratch[m:]
    flat, probes_ref, part, head, rest, head_sum, rest_sum, sk, probes_sem, own_sem, send_sem, recv_sem, *scratch = scratch
    place = Place(n_pts, n_hrs)
    me = place.pts * n_hrs + place.hrs
    rows = fields_ref.shape[0]
    local = sum(widths)
    k, hours = part.shape

    def split_id(o):
        t = lax.rem(me + o, n)
        return t, t // n_hrs, lax.rem(t, n_hrs)

    probes_load = pltpu.make_async_copy(probes_hbm, probes_ref, probes_sem)
    probes_load.start()
    barrier = pltpu.get_barrier_semaphore()

    @pl.loop(1, n)
    def _(o):
        _, tp, th = split_id(o)
        pl.semaphore_signal(barrier, inc=1, device_id=(tp, th), device_id_type=MESH)

    pl.semaphore_wait(barrier, n - 1)

    starts = [sum(widths[:c]) for c in range(m)]

    def source(t, c):
        return fields_ref.at[:, pl.ds(pl.multiple_of(t * local + starts[c], 128), widths[c])]

    owns = []
    for c in range(m):
        @pl.loop(1, n)
        def _(o):
            t, tp, th = split_id(o)
            pltpu.make_async_remote_copy(
                src_ref=source(t, c), dst_ref=panels[c].at[me], send_sem=send_sem.at[c], recv_sem=recv_sem.at[c],
                device_id=(tp, th), device_id_type=MESH,
            ).start()

        own = pltpu.make_async_copy(source(me, c), panels[c].at[me], own_sem.at[c])
        own.start()
        owns.append(own)

    heads = AllReduce(place, head, head_sum, 1, 1.0 / n_points, scratch[:10])
    rests = AllReduce(place, rest, rest_sum, 1, 1.0 / n_points, scratch[10:20])
    crosses = AllReduce(place, part, cross_ref, parts, 1.0 / n_points, scratch[20:])
    for ref, used in ((head, k // 4), (rest, k // 2)):
        if ref.shape[0] > used:
            ref[used:, :] = jnp.zeros((ref.shape[0] - used, k), jnp.float32)
    probes_load.wait()
    for c in range(m):
        owns[c].wait()
        most = panels[c].at[pl.ds(0, n - 1)]
        pltpu.make_async_copy(most, most, recv_sem.at[c]).wait()
        width = widths[c]
        cols = pl.ds(starts[c], width)
        if rows % 8 == 0:
            block = panels[c][...].reshape(n * rows, width)
        else:
            for d in range(n):
                flat[d * rows:(d + 1) * rows, :width] = panels[c][d]
            block = flat[:, :width]
        sketch = mm(probes_ref[...], block, ((1,), (0,)))
        sk[:, cols] = sketch
        pack(mm(sketch, sketch, ((1,), (1,))), head, rest, c == 0)
        if c == m - 1:
            heads.run(heads.cores)
            rests.run(rests.cores)
        if c < m - 1:
            term = mm(sketch, block, ((1,), (1,)))
            part[...] = term if c == 0 else part[...] + term
        else:
            span = n // crosses.place.cores
            for own in range(crosses.place.cores):
                core = lax.rem(crosses.place.core + 1 + own, crosses.place.cores)
                lanes = pl.ds(pl.multiple_of(core * span * rows, 128), span * rows)
                if rows % 8 == 0:
                    block = panels[c][pl.ds(core * span, span)].reshape(span * rows, width)
                else:
                    block = flat[pl.ds(pl.multiple_of(core * span * rows, 8), span * rows), :width]
                term = mm(sketch, block, ((1,), (1,)))
                part[:, lanes] = term if c == 0 else part[:, lanes] + term
                if own == 0:
                    crosses.run(crosses.cores)
    heads.run(heads.chips)
    rests.run(rests.chips)
    crosses.run(crosses.chips)
    heads.run(heads.layers)
    rests.run(rests.layers)
    crosses.run(crosses.layers)
    heads.run(heads.spread)
    rests.run(rests.spread)
    heads.run(heads.share)
    heads.finish()
    todo = {(0, 3): [functools.partial(rests.share, 0)], (0, -1): [rests.finish]}
    steps = [functools.partial(crosses.spread, p) for p in range(parts)] + [functools.partial(crosses.share, p) for p in range(parts)]
    for point, step in zip(POINTS, steps):
        todo.setdefault(point, []).append(step)

    def between(block, panel):
        if (block, panel) in todo:
            for step in todo[block, panel]:
                step()

    factor(head_sum, rest_sum, w_ref, between)
    step = 512
    for t in range(0, local, step):
        y_ref[:, t:t + step] = mm(w_ref[...], sk[:, t:t + step], ((1,), (0,)))
    crosses.finish()
    heads.drain()
    rests.drain()
    crosses.drain()
    for c in range(m):
        most = panels[c].at[pl.ds(0, n - 1)]
        pltpu.make_async_copy(most, most, send_sem.at[c]).wait()


def gather(fields, probes, n_pts, n_hrs):
    k, hours = probes.shape
    rows, n_points = fields.shape
    n = n_pts * n_hrs
    local = n_points // n
    widths = pieces(local)
    m = len(widths)
    cores, low, chips, layers = split(n_pts, n_hrs)
    parts = 2 if k % (2 * chips * 8) == 0 else 1
    sizes = (padded(k // 4, chips), padded(k // 2, chips))
    v = pl.BlockSpec(memory_space=pltpu.VMEM)
    far = pl.BlockSpec(memory_space=pltpu.HBM)
    dma = pltpu.SemaphoreType.DMA
    f32 = jnp.float32
    return pl.pallas_call(
        functools.partial(gather_kernel, n_pts, n_hrs, widths, parts, n_points),
        out_shape=(
            jax.ShapeDtypeStruct((k, local), f32), jax.ShapeDtypeStruct((k, k), f32), jax.ShapeDtypeStruct((k, hours), f32),
        ),
        in_specs=[far, far],
        out_specs=(v, v, v),
        scratch_shapes=[
            *(pltpu.VMEM((n, rows, width), f32) for width in widths),
            pltpu.VMEM((hours, max(widths)) if rows % 8 else (8, 128), f32),
            pltpu.VMEM((k, hours), f32),
            pltpu.VMEM((k, hours), f32),
            *(pltpu.VMEM((size, k), f32) for size in sizes * 2),
            pltpu.VMEM((k, local), f32),
            dma(()), dma((m,)), dma((m,)), dma((m,)),
            *(shape for size in sizes for shape in reduce_shapes(n_pts, n_hrs, size, k, 1)),
            *reduce_shapes(n_pts, n_hrs, k, hours, parts),
        ],
        compiler_params=pltpu.CompilerParams(collective_id=1, has_side_effects=True, vmem_limit_bytes=VMEM_LIMIT),
        name="gather",
    )(fields, probes)


def pieces(local):
    if local % 128 or local < 1024:
        return (local,)
    last = 256
    big = 512
    rest = local - last
    widths = []
    while rest > big:
        widths.append(big)
        rest -= big
    return (*widths, rest, last)


def on_device(fields, probes):
    n_pts = lax.axis_size("pts")
    n_hrs = lax.axis_size("hrs")
    y, w, cross = gather(pltpu.with_memory_space_constraint(fields, pltpu.HBM), pltpu.with_memory_space_constraint(probes, pltpu.HBM), n_pts, n_hrs)
    return finish(w, cross, y)


def solution(mesh):
    return jax.shard_map(
        on_device,
        mesh=mesh,
        in_specs=(P(("pts", "hrs"), None), P()),
        out_specs=(P(None, ("pts", "hrs")), P()),
        check_vma=False,
    )
```

```python
import functools

import jax
import jax.numpy as jnp
from jax import lax
from jax.experimental import pallas as pl
from jax.experimental.pallas import tpu as pltpu
from jax.sharding import PartitionSpec as P

HI = lax.Precision.HIGHEST
MESH = pl.DeviceIdType.MESH
VMEM_LIMIT = 24 * 2 ** 20
POINTS = ((0, 1), (0, 7), (1, 4), (1, 14))


def mm(a, b, dims):
    return lax.dot_general(a, b, (dims, ((), ())), precision=HI, preferred_element_type=jnp.float32)


def invert_block(block, between=None):
    b = block.shape[0]
    n = b // 8
    shape = (8, b)
    srow = lax.broadcasted_iota(jnp.int32, shape, 0)
    lane = lax.broadcasted_iota(jnp.int32, shape, 1)
    strips = [block[8 * s:8 * s + 8] for s in range(n)]
    diag = sum(jnp.where(lane == srow + 8 * s, strips[s], 0.0) for s in range(n))
    diag = jnp.broadcast_to(jnp.sum(diag, axis=0, keepdims=True), shape)
    col = 1.0 / diag
    root = lax.rsqrt(diag)
    strips = [strip * col for strip in strips]
    outs = [jnp.zeros(shape, jnp.float32)] * n

    def row_of(x, r):
        return jnp.broadcast_to(x[r:r + 1], shape)

    def spread(x, c, apart=True):
        x = jnp.broadcast_to(x[:, c:c + 1], shape)
        return jnp.maximum(x, -3e38) if apart else x

    for s0 in range(n):
        j = 8 * s0
        if between is not None:
            between(s0)
        panel = {s: [spread(strips[s], j + c, s == s0) for c in range(8)] for s in range(s0, n)}
        roots = [spread(root, j + c) for c in range(8)]
        inside = (lane >= j) & (lane < j + 8)
        for s in range(s0, n):
            unit = jnp.where(lane == srow + j, 1.0, 0.0) if s == s0 else 0.0
            strips[s] = jnp.where(inside, unit, strips[s])
        head = panel[s0]
        for p in range(0, 8, 2):
            a, b12 = row_of(head[p], p), row_of(head[p + 1], p)
            b21, c = row_of(head[p], p + 1), row_of(head[p + 1], p + 1)
            det = a * c - b12 * b21
            inv = 1.0 / det
            inva = 1.0 / a
            row1, row2 = row_of(strips[s0], p), row_of(strips[s0], p + 1)
            w1 = row1 * (lax.rsqrt(a) * roots[p])
            w2 = (row2 - (b21 * inva) * row1) * (lax.rsqrt(det * inva) * roots[p + 1])
            outs[s0] = jnp.where(srow == p, w1, jnp.where(srow == p + 1, w2, outs[s0]))
            v1, v2 = (c * row1 - b12 * row2) * inv, (a * row2 - b21 * row1) * inv
            y = {}
            for q in range(p + 2, 8):
                e1, e2 = row_of(head[q], p), row_of(head[q], p + 1)
                y[q] = (c * e1 - b12 * e2, a * e2 - b21 * e1)
            z = {q: (y[q][0] * inv, y[q][1] * inv) for q in y}
            for s in range(s0 if p < 6 else s0 + 1, n):
                f = panel[s]
                for q in range(p + 2, 8):
                    if s < s0 + 2:
                        f[q] = f[q] - (f[p] * y[q][0] + f[p + 1] * y[q][1]) * inv
                    else:
                        f[q] = f[q] - f[p] * z[q][0] - f[p + 1] * z[q][1]
                strips[s] = strips[s] - f[p] * v1 - f[p + 1] * v2
    return jnp.concatenate([jnp.where(lane <= srow + 8 * s, outs[s], 0.0) for s in range(n)], axis=0)


def padded(rows, chips):
    return -(-rows // (8 * chips)) * 8 * chips


def pack(g, head, rest, first):
    k = g.shape[0]
    h, q = k // 2, k // 4
    for ref, rows, cols, block in (
        (head, slice(0, q), slice(0, h), g[:q, :h]),
        (head, slice(0, q), slice(h, k), g[q:h, :h]),
        (rest, slice(0, h), slice(0, h), g[h:, h:]),
        (rest, slice(0, h), slice(h, k), g[h:, :h]),
    ):
        ref[rows, cols] = block if first else ref[rows, cols] + block


def factor(head, rest, w, between):
    k = w.shape[0]
    h, q = k // 2, k // 4
    first = jnp.concatenate([head[:q, :h], head[:q, h:]], axis=0)
    top = invert_block(first, functools.partial(between, 0))
    w[:h, :h] = top
    w[:h, h:] = jnp.zeros((h, k - h), jnp.float32)
    between(0, -1)
    side = mm(rest[:h, h:], top, ((1,), (1,)))
    second = rest[:h, :h] - mm(side, side, ((1,), (1,)))
    w[h:, :h] = mm(side, top, ((1,), (0,)))
    last = invert_block(second, functools.partial(between, 1))
    w[h:, h:] = last
    w[h:, :h] = -mm(last, w[h:, :h], ((1,), (0,)))


def output_kernel(w, cross, y, basis, coeffs, z, sem):
    first = pltpu.make_async_copy(y, basis, sem.at[0])
    first.start()
    z[...] = mm(w[...], cross[...], ((1,), (0,)))
    second = pltpu.make_async_copy(z, coeffs, sem.at[1])
    second.start()
    first.wait()
    second.wait()


def finish(w, cross, y):
    v = pl.BlockSpec(memory_space=pltpu.VMEM)
    hbm = pl.BlockSpec(memory_space=pl.ANY)
    f32 = jnp.float32
    return pl.pallas_call(
        output_kernel,
        out_shape=(jax.ShapeDtypeStruct(y.shape, f32), jax.ShapeDtypeStruct(cross.shape, f32)),
        in_specs=[v, v, v],
        out_specs=(hbm, hbm),
        scratch_shapes=[pltpu.VMEM(cross.shape, f32), pltpu.SemaphoreType.DMA((2,))],
        compiler_params=pltpu.CompilerParams(vmem_limit_bytes=VMEM_LIMIT),
        name="output",
    )(w, cross, y)


class Place:
    def __init__(self, n_pts, n_hrs, pair):
        self.pts, self.hrs = lax.axis_index("pts"), lax.axis_index("hrs")
        self.n_pts, self.n_hrs = n_pts, n_hrs
        self.cores, self.low, self.chips, self.layers = split(n_pts, n_hrs, pair)
        self.core = lax.rem(self.hrs, self.cores)
        self.layer = self.pts // self.low
        self.chip = (self.hrs // self.cores) * self.low + lax.rem(self.pts, self.low)

    def at(self, core, chip, layer):
        return (layer * self.low + lax.rem(chip, self.low), (chip // self.low) * self.cores + core)


def split(n_pts, n_hrs, pair):
    cores = 2 if pair and n_hrs % 2 == 0 else 1
    low = 1
    while n_pts % (low * 2) == 0 and low * 2 * low * 2 <= n_pts:
        low *= 2
    return cores, low, (n_hrs // cores) * low, n_pts // low


def reduce_shapes(n_pts, n_hrs, pair, rows, width, parts):
    cores, low, chips, layers = split(n_pts, n_hrs, pair)
    lanes = width // cores
    h = rows // parts
    q = h // chips
    f32 = jnp.float32
    dma = pltpu.SemaphoreType.DMA
    return [
        pltpu.VMEM((parts, h, lanes), f32),
        pltpu.VMEM((parts, h, lanes), f32),
        pltpu.VMEM((parts, max(chips - 1, 1), q, lanes), f32),
        pltpu.VMEM((parts, layers, q, lanes), f32),
        dma((parts, 2)), dma((parts, 2)),
        dma((parts, 2, max(chips - 1, 1))), dma((parts, 2, max(chips - 1, 1))),
        dma((parts, max(layers - 1, 1))), dma((parts, max(layers - 1, 1))),
    ]


class AllReduce:
    def __init__(self, place, x, out, parts, scale, scratch):
        self.place, self.x, self.out, self.parts, self.scale = place, x, out, parts, scale
        self.got1, self.sum1, self.got2, self.sums, self.s1, self.r1, self.s2, self.r2, self.s3, self.r3 = scratch
        self.h, self.lanes = self.got1.shape[1], self.got1.shape[2]
        self.q = self.sums.shape[2]
        self.started = []
        self.copies = {}

    def send(self, key, src, dst, ss, rs, device):
        copy = pltpu.make_async_remote_copy(
            src_ref=src, dst_ref=dst, send_sem=ss, recv_sem=rs, device_id=device, device_id_type=MESH)
        copy.start()
        self.started.append(copy)
        self.copies.setdefault(key, []).append(copy)

    def arrived(self, key):
        for copy in self.copies.get(key, ()):
            copy.wait_recv()

    def half(self, core, p):
        return pl.ds(p * self.h, self.h), pl.ds(pl.multiple_of(core * self.lanes, 128), self.lanes)

    def piece(self, chip):
        return pl.ds(pl.multiple_of(chip * self.q, 8), self.q)

    def cores(self, p):
        at = self.place
        if at.cores > 1:
            other = 1 - at.core
            self.send((1, p), self.x.at[self.half(other, p)], self.got1.at[p], self.s1.at[p, 0], self.r1.at[p, 0],
                      at.at(other, at.chip, at.layer))

    def chips(self, p):
        at = self.place
        self.arrived((1, p))
        mine = self.x[self.half(at.core, p)]
        self.sum1[p] = mine + self.got1[p] if at.cores > 1 else mine
        for o in range(1, at.chips):
            chip = lax.rem(at.chip + o, at.chips)
            self.send((2, p), self.sum1.at[p, self.piece(chip)], self.got2.at[p, o - 1], self.s2.at[p, 0, o - 1], self.r2.at[p, 0, o - 1],
                      at.at(at.core, chip, at.layer))

    def layers(self, p):
        at = self.place
        self.arrived((2, p))
        total = self.sum1[p, self.piece(at.chip)]
        for o in range(1, at.chips):
            total = total + self.got2[p, o - 1]
        self.sums[p, at.layer] = total
        for o in range(1, at.layers):
            layer = lax.rem(at.layer + o, at.layers)
            self.send((3, p), self.sums.at[p, at.layer], self.sums.at[p, at.layer], self.s3.at[p, o - 1], self.r3.at[p, o - 1],
                      at.at(at.core, at.chip, layer))

    def spread(self, p):
        at = self.place
        self.arrived((3, p))
        total = self.sums[p, 0]
        for layer in range(1, at.layers):
            total = total + self.sums[p, layer]
        rows, lanes = self.half(at.core, p)
        block = (pl.ds(pl.multiple_of(p * self.h + at.chip * self.q, 8), self.q), lanes)
        self.out[block] = total * self.scale
        for o in range(1, at.chips):
            chip = lax.rem(at.chip + o, at.chips)
            self.send((4, p), self.out.at[block], self.out.at[block], self.s2.at[p, 1, o - 1], self.r2.at[p, 1, o - 1],
                      at.at(at.core, chip, at.layer))

    def share(self, p):
        at = self.place
        self.arrived((4, p))
        if at.cores > 1:
            half = self.half(at.core, p)
            self.send((5, p), self.out.at[half], self.out.at[half], self.s1.at[p, 1], self.r1.at[p, 1],
                      at.at(1 - at.core, at.chip, at.layer))

    def run(self, step):
        for p in range(self.parts):
            step(p)

    def finish(self):
        for p in range(self.parts):
            self.arrived((5, p))

    def drain(self):
        for copy in self.started:
            copy.wait_send()


def gather_kernel(n_pts, n_hrs, widths, parts, n_points, fields_ref, probes_hbm, y_ref, w_ref, cross_ref, *scratch):
    n = n_pts * n_hrs
    m = len(widths)
    panels, scratch = scratch[:m], scratch[m:]
    flat, probes_ref, part, head, rest, head_sum, rest_sum, sk, probes_sem, own_sem, send_sem, recv_sem, *scratch = scratch
    place = Place(n_pts, n_hrs, True)
    me = place.pts * n_hrs + place.hrs
    rows = fields_ref.shape[0]
    local = sum(widths)
    k, hours = part.shape

    def split_id(o):
        t = lax.rem(me + o, n)
        return t, t // n_hrs, lax.rem(t, n_hrs)

    probes_load = pltpu.make_async_copy(probes_hbm, probes_ref, probes_sem)
    probes_load.start()
    barrier = pltpu.get_barrier_semaphore()

    @pl.loop(1, n)
    def _(o):
        _, tp, th = split_id(o)
        pl.semaphore_signal(barrier, inc=1, device_id=(tp, th), device_id_type=MESH)

    pl.semaphore_wait(barrier, n - 1)

    starts = [sum(widths[:c]) for c in range(m)]

    def source(t, c):
        return fields_ref.at[:, pl.ds(pl.multiple_of(t * local + starts[c], 128), widths[c])]

    owns = []
    for c in range(m):
        @pl.loop(1, n)
        def _(o):
            t, tp, th = split_id(o)
            pltpu.make_async_remote_copy(
                src_ref=source(t, c), dst_ref=panels[c].at[me], send_sem=send_sem.at[c], recv_sem=recv_sem.at[c],
                device_id=(tp, th), device_id_type=MESH,
            ).start()

        own = pltpu.make_async_copy(source(me, c), panels[c].at[me], own_sem.at[c])
        own.start()
        owns.append(own)

    heads = AllReduce(Place(n_pts, n_hrs, False), head, head_sum, 1, 1.0 / n_points, scratch[:10])
    rests = AllReduce(place, rest, rest_sum, 1, 1.0 / n_points, scratch[10:20])
    crosses = AllReduce(place, part, cross_ref, parts, 1.0 / n_points, scratch[20:])
    for ref, used in ((head, k // 4), (rest, k // 2)):
        if ref.shape[0] > used:
            ref[used:, :] = jnp.zeros((ref.shape[0] - used, k), jnp.float32)
    probes_load.wait()
    for c in range(m):
        owns[c].wait()
        most = panels[c].at[pl.ds(0, n - 1)]
        pltpu.make_async_copy(most, most, recv_sem.at[c]).wait()
        width = widths[c]
        cols = pl.ds(starts[c], width)
        if rows % 8 == 0:
            block = panels[c][...].reshape(n * rows, width)
        else:
            for d in range(n):
                flat[d * rows:(d + 1) * rows, :width] = panels[c][d]
            block = flat[:, :width]
        sketch = mm(probes_ref[...], block, ((1,), (0,)))
        sk[:, cols] = sketch
        pack(mm(sketch, sketch, ((1,), (1,))), head, rest, c == 0)
        if c == m - 1:
            heads.run(heads.chips)
            rests.run(rests.cores)
        if c < m - 1:
            term = mm(sketch, block, ((1,), (1,)))
            part[...] = term if c == 0 else part[...] + term
        else:
            span = n // crosses.place.cores
            for own in range(crosses.place.cores):
                core = lax.rem(crosses.place.core + 1 + own, crosses.place.cores)
                lanes = pl.ds(pl.multiple_of(core * span * rows, 128), span * rows)
                if rows % 8 == 0:
                    block = panels[c][pl.ds(core * span, span)].reshape(span * rows, width)
                else:
                    block = flat[pl.ds(pl.multiple_of(core * span * rows, 8), span * rows), :width]
                term = mm(sketch, block, ((1,), (1,)))
                part[:, lanes] = term if c == 0 else part[:, lanes] + term
                if own == 0:
                    crosses.run(crosses.cores)
    rests.run(rests.chips)
    crosses.run(crosses.chips)
    heads.run(heads.layers)
    rests.run(rests.layers)
    crosses.layers(0)
    heads.run(heads.spread)
    for p in range(1, parts):
        crosses.layers(p)
    rests.run(rests.spread)
    heads.run(heads.share)
    heads.finish()
    todo = {(0, 3): [functools.partial(rests.share, 0)], (0, -1): [rests.finish]}
    steps = [functools.partial(crosses.spread, p) for p in range(parts)] + [functools.partial(crosses.share, p) for p in range(parts)]
    for point, step in zip(POINTS, steps):
        todo.setdefault(point, []).append(step)

    def between(block, panel):
        if (block, panel) in todo:
            for step in todo[block, panel]:
                step()

    factor(head_sum, rest_sum, w_ref, between)
    step = 512
    for t in range(0, local, step):
        y_ref[:, t:t + step] = mm(w_ref[...], sk[:, t:t + step], ((1,), (0,)))
    crosses.finish()
    heads.drain()
    rests.drain()
    crosses.drain()
    for c in range(m):
        most = panels[c].at[pl.ds(0, n - 1)]
        pltpu.make_async_copy(most, most, send_sem.at[c]).wait()


def gather(fields, probes, n_pts, n_hrs):
    k, hours = probes.shape
    rows, n_points = fields.shape
    n = n_pts * n_hrs
    local = n_points // n
    widths = pieces(local)
    m = len(widths)
    _, _, chips, _ = split(n_pts, n_hrs, True)
    parts = 2 if k % (2 * chips * 8) == 0 else 1
    sizes = (padded(k // 4, split(n_pts, n_hrs, False)[2]), padded(k // 2, chips))
    v = pl.BlockSpec(memory_space=pltpu.VMEM)
    far = pl.BlockSpec(memory_space=pltpu.HBM)
    dma = pltpu.SemaphoreType.DMA
    f32 = jnp.float32
    return pl.pallas_call(
        functools.partial(gather_kernel, n_pts, n_hrs, widths, parts, n_points),
        out_shape=(
            jax.ShapeDtypeStruct((k, local), f32), jax.ShapeDtypeStruct((k, k), f32), jax.ShapeDtypeStruct((k, hours), f32),
        ),
        in_specs=[far, far],
        out_specs=(v, v, v),
        scratch_shapes=[
            *(pltpu.VMEM((n, rows, width), f32) for width in widths),
            pltpu.VMEM((hours, max(widths)) if rows % 8 else (8, 128), f32),
            pltpu.VMEM((k, hours), f32),
            pltpu.VMEM((k, hours), f32),
            *(pltpu.VMEM((size, k), f32) for size in sizes * 2),
            pltpu.VMEM((k, local), f32),
            dma(()), dma((m,)), dma((m,)), dma((m,)),
            *reduce_shapes(n_pts, n_hrs, False, sizes[0], k, 1),
            *reduce_shapes(n_pts, n_hrs, True, sizes[1], k, 1),
            *reduce_shapes(n_pts, n_hrs, True, k, hours, parts),
        ],
        compiler_params=pltpu.CompilerParams(collective_id=1, has_side_effects=True, vmem_limit_bytes=VMEM_LIMIT),
        name="gather",
    )(fields, probes)


def pieces(local):
    if local % 128 or local < 1024:
        return (local,)
    last = 256
    big = 512
    rest = local - last
    widths = []
    while rest > big:
        widths.append(big)
        rest -= big
    return (*widths, rest, last)


def on_device(fields, probes):
    n_pts = lax.axis_size("pts")
    n_hrs = lax.axis_size("hrs")
    y, w, cross = gather(pltpu.with_memory_space_constraint(fields, pltpu.HBM), pltpu.with_memory_space_constraint(probes, pltpu.HBM), n_pts, n_hrs)
    return finish(w, cross, y)


def solution(mesh):
    return jax.shard_map(
        on_device,
        mesh=mesh,
        in_specs=(P(("pts", "hrs"), None), P()),
        out_specs=(P(None, ("pts", "hrs")), P()),
        check_vma=False,
    )
```

```python
import functools

import jax
import jax.numpy as jnp
from jax import lax
from jax.experimental import pallas as pl
from jax.experimental.pallas import tpu as pltpu
from jax.sharding import PartitionSpec as P

HI = lax.Precision.HIGHEST
MESH = pl.DeviceIdType.MESH
VMEM_LIMIT = 24 * 2 ** 20
POINTS = ((0, 1), (0, 7), (1, 4), (1, 14))


def mm(a, b, dims):
    return lax.dot_general(a, b, (dims, ((), ())), precision=HI, preferred_element_type=jnp.float32)


def invert_block(block, between=None):
    b = block.shape[0]
    n = b // 8
    shape = (8, b)
    srow = lax.broadcasted_iota(jnp.int32, shape, 0)
    lane = lax.broadcasted_iota(jnp.int32, shape, 1)
    strips = [block[8 * s:8 * s + 8] for s in range(n)]
    diag = sum(jnp.where(lane == srow + 8 * s, strips[s], 0.0) for s in range(n))
    diag = jnp.broadcast_to(jnp.sum(diag, axis=0, keepdims=True), shape)
    col = 1.0 / diag
    root = lax.rsqrt(diag)
    strips = [strip * col for strip in strips]
    outs = [jnp.zeros(shape, jnp.float32)] * n

    def row_of(x, r):
        return jnp.broadcast_to(x[r:r + 1], shape)

    def spread(x, c, apart=True):
        x = jnp.broadcast_to(x[:, c:c + 1], shape)
        return jnp.maximum(x, -3e38) if apart else x

    for s0 in range(n):
        j = 8 * s0
        if between is not None:
            between(s0)
        panel = {s: [spread(strips[s], j + c, s == s0) for c in range(8)] for s in range(s0, n)}
        roots = [spread(root, j + c) for c in range(8)]
        inside = (lane >= j) & (lane < j + 8)
        for s in range(s0, n):
            unit = jnp.where(lane == srow + j, 1.0, 0.0) if s == s0 else 0.0
            strips[s] = jnp.where(inside, unit, strips[s])
        head = panel[s0]
        for p in range(0, 8, 2):
            a, b12 = row_of(head[p], p), row_of(head[p + 1], p)
            b21, c = row_of(head[p], p + 1), row_of(head[p + 1], p + 1)
            det = a * c - b12 * b21
            inv = 1.0 / det
            inva = 1.0 / a
            row1, row2 = row_of(strips[s0], p), row_of(strips[s0], p + 1)
            w1 = row1 * (lax.rsqrt(a) * roots[p])
            w2 = (row2 - (b21 * inva) * row1) * (lax.rsqrt(det * inva) * roots[p + 1])
            outs[s0] = jnp.where(srow == p, w1, jnp.where(srow == p + 1, w2, outs[s0]))
            v1, v2 = (c * row1 - b12 * row2) * inv, (a * row2 - b21 * row1) * inv
            y = {}
            for q in range(p + 2, 8):
                e1, e2 = row_of(head[q], p), row_of(head[q], p + 1)
                y[q] = (c * e1 - b12 * e2, a * e2 - b21 * e1)
            z = {q: (y[q][0] * inv, y[q][1] * inv) for q in y}
            for s in range(s0 if p < 6 else s0 + 1, n):
                f = panel[s]
                for q in range(p + 2, 8):
                    if s < s0 + 2:
                        f[q] = f[q] - (f[p] * y[q][0] + f[p + 1] * y[q][1]) * inv
                    else:
                        f[q] = f[q] - f[p] * z[q][0] - f[p + 1] * z[q][1]
                strips[s] = strips[s] - f[p] * v1 - f[p + 1] * v2
    return jnp.concatenate([jnp.where(lane <= srow + 8 * s, outs[s], 0.0) for s in range(n)], axis=0)


def padded(rows, chips):
    return -(-rows // (8 * chips)) * 8 * chips


def add_to(ref, blocks, first):
    for rows, cols, block in blocks:
        ref[rows, cols] = block if first else ref[rows, cols] + block


def add_head(sketch, head, first):
    k = sketch.shape[0]
    h, q = k // 2, k // 4
    g = mm(sketch[:h], sketch[:h], ((1,), (1,)))
    add_to(head, ((slice(0, q), slice(0, h), g[:q]), (slice(0, q), slice(h, k), g[q:])), first)


def add_rest(sketch, rest, first):
    k = sketch.shape[0]
    h = k // 2
    g = mm(sketch[h:], sketch, ((1,), (1,)))
    add_to(rest, ((slice(0, h), slice(0, h), g[:, h:]), (slice(0, h), slice(h, k), g[:, :h])), first)


def factor(head, rest, w, between):
    k = w.shape[0]
    h, q = k // 2, k // 4
    first = jnp.concatenate([head[:q, :h], head[:q, h:]], axis=0)
    top = invert_block(first, functools.partial(between, 0))
    w[:h, :h] = top
    w[:h, h:] = jnp.zeros((h, k - h), jnp.float32)
    between(0, -1)
    side = mm(rest[:h, h:], top, ((1,), (1,)))
    second = rest[:h, :h] - mm(side, side, ((1,), (1,)))
    w[h:, :h] = mm(side, top, ((1,), (0,)))
    last = invert_block(second, functools.partial(between, 1))
    w[h:, h:] = last
    w[h:, :h] = -mm(last, w[h:, :h], ((1,), (0,)))


def output_kernel(w, cross, y, basis, coeffs, z, sem):
    first = pltpu.make_async_copy(y, basis, sem.at[0])
    first.start()
    z[...] = mm(w[...], cross[...], ((1,), (0,)))
    second = pltpu.make_async_copy(z, coeffs, sem.at[1])
    second.start()
    first.wait()
    second.wait()


def finish(w, cross, y):
    v = pl.BlockSpec(memory_space=pltpu.VMEM)
    hbm = pl.BlockSpec(memory_space=pl.ANY)
    f32 = jnp.float32
    return pl.pallas_call(
        output_kernel,
        out_shape=(jax.ShapeDtypeStruct(y.shape, f32), jax.ShapeDtypeStruct(cross.shape, f32)),
        in_specs=[v, v, v],
        out_specs=(hbm, hbm),
        scratch_shapes=[pltpu.VMEM(cross.shape, f32), pltpu.SemaphoreType.DMA((2,))],
        compiler_params=pltpu.CompilerParams(vmem_limit_bytes=VMEM_LIMIT),
        name="output",
    )(w, cross, y)


class Place:
    def __init__(self, n_pts, n_hrs, pair):
        self.pts, self.hrs = lax.axis_index("pts"), lax.axis_index("hrs")
        self.n_pts, self.n_hrs = n_pts, n_hrs
        self.cores, self.low, self.chips, self.layers = split(n_pts, n_hrs, pair)
        self.core = lax.rem(self.hrs, self.cores)
        self.layer = self.pts // self.low
        self.chip = (self.hrs // self.cores) * self.low + lax.rem(self.pts, self.low)

    def at(self, core, chip, layer):
        return (layer * self.low + lax.rem(chip, self.low), (chip // self.low) * self.cores + core)


def split(n_pts, n_hrs, pair):
    cores = 2 if pair and n_hrs % 2 == 0 else 1
    low = 1
    while n_pts % (low * 2) == 0 and low * 2 * low * 2 <= n_pts:
        low *= 2
    return cores, low, (n_hrs // cores) * low, n_pts // low


def reduce_shapes(n_pts, n_hrs, pair, rows, width, parts):
    cores, low, chips, layers = split(n_pts, n_hrs, pair)
    lanes = width // cores
    h = rows // parts
    q = h // chips
    f32 = jnp.float32
    dma = pltpu.SemaphoreType.DMA
    return [
        pltpu.VMEM((parts, h, lanes), f32),
        pltpu.VMEM((parts, h, lanes), f32),
        pltpu.VMEM((parts, max(chips - 1, 1), q, lanes), f32),
        pltpu.VMEM((parts, layers, q, lanes), f32),
        dma((parts, 2)), dma((parts, 2)),
        dma((parts, 2, max(chips - 1, 1))), dma((parts, 2, max(chips - 1, 1))),
        dma((parts, max(layers - 1, 1))), dma((parts, max(layers - 1, 1))),
    ]


class AllReduce:
    def __init__(self, place, x, out, parts, scale, scratch):
        self.place, self.x, self.out, self.parts, self.scale = place, x, out, parts, scale
        self.got1, self.sum1, self.got2, self.sums, self.s1, self.r1, self.s2, self.r2, self.s3, self.r3 = scratch
        self.h, self.lanes = self.got1.shape[1], self.got1.shape[2]
        self.q = self.sums.shape[2]
        self.started = []
        self.copies = {}

    def send(self, key, src, dst, ss, rs, device):
        copy = pltpu.make_async_remote_copy(
            src_ref=src, dst_ref=dst, send_sem=ss, recv_sem=rs, device_id=device, device_id_type=MESH)
        copy.start()
        self.started.append(copy)
        self.copies.setdefault(key, []).append(copy)

    def arrived(self, key):
        for copy in self.copies.get(key, ()):
            copy.wait_recv()

    def half(self, core, p):
        return pl.ds(p * self.h, self.h), pl.ds(pl.multiple_of(core * self.lanes, 128), self.lanes)

    def piece(self, chip):
        return pl.ds(pl.multiple_of(chip * self.q, 8), self.q)

    def cores(self, p):
        at = self.place
        if at.cores > 1:
            other = 1 - at.core
            self.send((1, p), self.x.at[self.half(other, p)], self.got1.at[p], self.s1.at[p, 0], self.r1.at[p, 0],
                      at.at(other, at.chip, at.layer))

    def chips(self, p):
        at = self.place
        self.arrived((1, p))
        mine = self.x[self.half(at.core, p)]
        self.sum1[p] = mine + self.got1[p] if at.cores > 1 else mine
        for o in range(1, at.chips):
            chip = lax.rem(at.chip + o, at.chips)
            self.send((2, p), self.sum1.at[p, self.piece(chip)], self.got2.at[p, o - 1], self.s2.at[p, 0, o - 1], self.r2.at[p, 0, o - 1],
                      at.at(at.core, chip, at.layer))

    def layers(self, p):
        at = self.place
        self.arrived((2, p))
        total = self.sum1[p, self.piece(at.chip)]
        for o in range(1, at.chips):
            total = total + self.got2[p, o - 1]
        self.sums[p, at.layer] = total
        for o in range(1, at.layers):
            layer = lax.rem(at.layer + o, at.layers)
            self.send((3, p), self.sums.at[p, at.layer], self.sums.at[p, at.layer], self.s3.at[p, o - 1], self.r3.at[p, o - 1],
                      at.at(at.core, at.chip, layer))

    def spread(self, p):
        at = self.place
        self.arrived((3, p))
        total = self.sums[p, 0]
        for layer in range(1, at.layers):
            total = total + self.sums[p, layer]
        rows, lanes = self.half(at.core, p)
        block = (pl.ds(pl.multiple_of(p * self.h + at.chip * self.q, 8), self.q), lanes)
        self.out[block] = total * self.scale
        for o in range(1, at.chips):
            chip = lax.rem(at.chip + o, at.chips)
            self.send((4, p), self.out.at[block], self.out.at[block], self.s2.at[p, 1, o - 1], self.r2.at[p, 1, o - 1],
                      at.at(at.core, chip, at.layer))

    def share(self, p):
        at = self.place
        self.arrived((4, p))
        if at.cores > 1:
            half = self.half(at.core, p)
            self.send((5, p), self.out.at[half], self.out.at[half], self.s1.at[p, 1], self.r1.at[p, 1],
                      at.at(1 - at.core, at.chip, at.layer))

    def run(self, step):
        for p in range(self.parts):
            step(p)

    def finish(self):
        for p in range(self.parts):
            self.arrived((5, p))

    def drain(self):
        for copy in self.started:
            copy.wait_send()


def gather_kernel(n_pts, n_hrs, widths, parts, n_points, fields_ref, probes_hbm, y_ref, w_ref, cross_ref, *scratch):
    n = n_pts * n_hrs
    m = len(widths)
    panels, scratch = scratch[:m], scratch[m:]
    flat, probes_ref, part, head, rest, head_sum, rest_sum, sk, probes_sem, own_sem, send_sem, recv_sem, *scratch = scratch
    place = Place(n_pts, n_hrs, True)
    me = place.pts * n_hrs + place.hrs
    rows = fields_ref.shape[0]
    local = sum(widths)
    k, hours = part.shape

    def split_id(o):
        t = lax.rem(me + o, n)
        return t, t // n_hrs, lax.rem(t, n_hrs)

    probes_load = pltpu.make_async_copy(probes_hbm, probes_ref, probes_sem)
    probes_load.start()
    barrier = pltpu.get_barrier_semaphore()

    @pl.loop(1, n)
    def _(o):
        _, tp, th = split_id(o)
        pl.semaphore_signal(barrier, inc=1, device_id=(tp, th), device_id_type=MESH)

    pl.semaphore_wait(barrier, n - 1)

    starts = [sum(widths[:c]) for c in range(m)]

    def source(t, c):
        return fields_ref.at[:, pl.ds(pl.multiple_of(t * local + starts[c], 128), widths[c])]

    owns = []
    for c in range(m):
        @pl.loop(1, n)
        def _(o):
            t, tp, th = split_id(o)
            pltpu.make_async_remote_copy(
                src_ref=source(t, c), dst_ref=panels[c].at[me], send_sem=send_sem.at[c], recv_sem=recv_sem.at[c],
                device_id=(tp, th), device_id_type=MESH,
            ).start()

        own = pltpu.make_async_copy(source(me, c), panels[c].at[me], own_sem.at[c])
        own.start()
        owns.append(own)

    heads = AllReduce(Place(n_pts, n_hrs, False), head, head_sum, 1, 1.0 / n_points, scratch[:10])
    rests = AllReduce(place, rest, rest_sum, 1, 1.0 / n_points, scratch[10:20])
    crosses = AllReduce(place, part, cross_ref, parts, 1.0 / n_points, scratch[20:])
    for ref, used in ((head, k // 4), (rest, k // 2)):
        if ref.shape[0] > used:
            ref[used:, :] = jnp.zeros((ref.shape[0] - used, k), jnp.float32)
    probes_load.wait()
    for c in range(m):
        owns[c].wait()
        most = panels[c].at[pl.ds(0, n - 1)]
        pltpu.make_async_copy(most, most, recv_sem.at[c]).wait()
        width = widths[c]
        cols = pl.ds(starts[c], width)
        if rows % 8 == 0:
            block = panels[c][...].reshape(n * rows, width)
        else:
            for d in range(n):
                flat[d * rows:(d + 1) * rows, :width] = panels[c][d]
            block = flat[:, :width]
        sketch = mm(probes_ref[...], block, ((1,), (0,)))
        sk[:, cols] = sketch
        add_head(sketch, head, c == 0)
        if c == m - 1:
            heads.run(heads.chips)
        add_rest(sketch, rest, c == 0)
        if c == m - 1:
            rests.run(rests.cores)
        if c < m - 1:
            term = mm(sketch, block, ((1,), (1,)))
            part[...] = term if c == 0 else part[...] + term
        else:
            span = n // crosses.place.cores
            for own in range(crosses.place.cores):
                core = lax.rem(crosses.place.core + 1 + own, crosses.place.cores)
                lanes = pl.ds(pl.multiple_of(core * span * rows, 128), span * rows)
                if rows % 8 == 0:
                    block = panels[c][pl.ds(core * span, span)].reshape(span * rows, width)
                else:
                    block = flat[pl.ds(pl.multiple_of(core * span * rows, 8), span * rows), :width]
                term = mm(sketch, block, ((1,), (1,)))
                part[:, lanes] = term if c == 0 else part[:, lanes] + term
                if own == 0:
                    crosses.run(crosses.cores)
    rests.run(rests.chips)
    crosses.run(crosses.chips)
    heads.run(heads.layers)
    rests.run(rests.layers)
    crosses.layers(0)
    heads.run(heads.spread)
    for p in range(1, parts):
        crosses.layers(p)
    rests.run(rests.spread)
    heads.run(heads.share)
    heads.finish()
    todo = {(0, 3): [functools.partial(rests.share, 0)], (0, -1): [rests.finish]}
    steps = [functools.partial(crosses.spread, p) for p in range(parts)] + [functools.partial(crosses.share, p) for p in range(parts)]
    for point, step in zip(POINTS, steps):
        todo.setdefault(point, []).append(step)

    def between(block, panel):
        if (block, panel) in todo:
            for step in todo[block, panel]:
                step()

    factor(head_sum, rest_sum, w_ref, between)
    step = 512
    for t in range(0, local, step):
        y_ref[:, t:t + step] = mm(w_ref[...], sk[:, t:t + step], ((1,), (0,)))
    crosses.finish()
    heads.drain()
    rests.drain()
    crosses.drain()
    for c in range(m):
        most = panels[c].at[pl.ds(0, n - 1)]
        pltpu.make_async_copy(most, most, send_sem.at[c]).wait()


def gather(fields, probes, n_pts, n_hrs):
    k, hours = probes.shape
    rows, n_points = fields.shape
    n = n_pts * n_hrs
    local = n_points // n
    widths = pieces(local)
    m = len(widths)
    _, _, chips, _ = split(n_pts, n_hrs, True)
    parts = 2 if k % (2 * chips * 8) == 0 else 1
    sizes = (padded(k // 4, split(n_pts, n_hrs, False)[2]), padded(k // 2, chips))
    v = pl.BlockSpec(memory_space=pltpu.VMEM)
    far = pl.BlockSpec(memory_space=pltpu.HBM)
    dma = pltpu.SemaphoreType.DMA
    f32 = jnp.float32
    return pl.pallas_call(
        functools.partial(gather_kernel, n_pts, n_hrs, widths, parts, n_points),
        out_shape=(
            jax.ShapeDtypeStruct((k, local), f32), jax.ShapeDtypeStruct((k, k), f32), jax.ShapeDtypeStruct((k, hours), f32),
        ),
        in_specs=[far, far],
        out_specs=(v, v, v),
        scratch_shapes=[
            *(pltpu.VMEM((n, rows, width), f32) for width in widths),
            pltpu.VMEM((hours, max(widths)) if rows % 8 else (8, 128), f32),
            pltpu.VMEM((k, hours), f32),
            pltpu.VMEM((k, hours), f32),
            *(pltpu.VMEM((size, k), f32) for size in sizes * 2),
            pltpu.VMEM((k, local), f32),
            dma(()), dma((m,)), dma((m,)), dma((m,)),
            *reduce_shapes(n_pts, n_hrs, False, sizes[0], k, 1),
            *reduce_shapes(n_pts, n_hrs, True, sizes[1], k, 1),
            *reduce_shapes(n_pts, n_hrs, True, k, hours, parts),
        ],
        compiler_params=pltpu.CompilerParams(collective_id=1, has_side_effects=True, vmem_limit_bytes=VMEM_LIMIT),
        name="gather",
    )(fields, probes)


def pieces(local):
    if local % 128 or local < 1024:
        return (local,)
    last = 256
    big = 512
    rest = local - last
    widths = []
    while rest > big:
        widths.append(big)
        rest -= big
    return (*widths, rest, last)


def on_device(fields, probes):
    n_pts = lax.axis_size("pts")
    n_hrs = lax.axis_size("hrs")
    y, w, cross = gather(pltpu.with_memory_space_constraint(fields, pltpu.HBM), pltpu.with_memory_space_constraint(probes, pltpu.HBM), n_pts, n_hrs)
    return finish(w, cross, y)


def solution(mesh):
    return jax.shard_map(
        on_device,
        mesh=mesh,
        in_specs=(P(("pts", "hrs"), None), P()),
        out_specs=(P(None, ("pts", "hrs")), P()),
        check_vma=False,
    )
```
